256 devices in a mesh: seq: 32 (over y, z), grp: 8 (over x, core).
Axes of the slice: x: 4, y: 4, z: 8, core: 2. Of those that a mesh axis runs over, the one named last changes fastest.
Arguments:
- event_codes: int32 [2097152], P(('seq', 'grp')), may hold values from 0 to 255
- window_ends: int32 [196608], P(('seq', 'grp')), may hold values from 0 to 8191, as said below
- window_count: int32 [256], P(('seq', 'grp')), may hold values from 1 to 768, as said below
- handed: int32 [256], P(('seq', 'grp')), may hold values from 0 to 256, as said below
Outputs:
- window_share: float32 [131072, 256], P(('seq', 'grp'))
- share_gap: float32 [131072, 256], P(('seq', 'grp'))
The draws below stay inside these ranges and needn't reach their ends.
Inputs may be any that keep to these rules, and one draw needn't show every extreme that they name: `window_ends`: for each shard, its first window_count slots hold distinct offsets in rising order; the remaining slots hold 0. `window_count`: some shard has 768 windows in every draw. `handed`: at most the shard's window_count minus 1; 0 on the last shard of each group along grp; the windows a shard keeps plus those it receives number at most 512, and exactly 512 on some shard that passes 512 // 2 in every draw.
All inputs are finite; a program needn't handle non-finite values.
Results may differ from the reference program's by a relative error of at most 0.0003.
Values sent between devices are 32-bit elements; how exact they have to be, the bound alone decides.
A program may use at most 64 MiB of HBM per device.

```python
import jax
import jax.numpy as jnp
from jax import lax

CODES = 256
WINDOW = 4096
SHARD = 8192
CAP = 512
SLOTS = 768
GROUP = 8
NSHARDS = 256
EVENTS = 2097152


def window_plan(key):
    shard_ids = jnp.arange(NSHARDS, dtype=jnp.int32)
    within = shard_ids % GROUP
    handed = jax.random.randint(jax.random.fold_in(key, 101), (NSHARDS,), 0, CAP // 2 + 1)
    handed = jnp.where(within == GROUP - 1, 0, handed)
    chosen = jax.random.randint(jax.random.fold_in(key, 103), (), 0, NSHARDS // GROUP) * GROUP
    chosen = chosen + jax.random.randint(jax.random.fold_in(key, 107), (), 0, GROUP - 1)
    handed = handed.at[(chosen + NSHARDS - 1) % NSHARDS].set(0)
    handed = handed.at[chosen].set(CAP // 2)
    received = jnp.where(within == 0, 0, jnp.roll(handed, 1))
    factor_one = jax.random.randint(jax.random.fold_in(key, 109), (NSHARDS,), 0, CAP)
    factor_two = jax.random.randint(jax.random.fold_in(key, 113), (NSHARDS,), 0, CAP)
    extra = factor_one * factor_two // CAP
    loaded = jnp.minimum(received + 1 + extra, CAP)
    loaded = loaded.at[chosen].set(CAP)
    return ((loaded - received + handed).astype(jnp.int32), handed.astype(jnp.int32))


def draw_event_codes(key, part):
    relabel = jax.random.permutation(jax.random.fold_in(key, 3), CODES)
    factor_one = jax.random.randint(jax.random.fold_in(key, 5), (EVENTS,), 0, CODES)
    factor_two = jax.random.randint(jax.random.fold_in(key, 7), (EVENTS,), 0, CODES)
    skewed = factor_one * factor_two // CODES
    moving = jnp.arange(EVENTS, dtype=jnp.int32) // SHARD * CODES // (2 * NSHARDS)
    return relabel[(skewed + moving) % CODES].astype(jnp.int32)


def draw_window_ends(key, part):
    counts = window_plan(key)[0]
    shard_keys = jax.random.split(jax.random.fold_in(key, 127), NSHARDS)
    picks = jax.vmap(lambda one_key: jax.random.permutation(one_key, SHARD)[:SLOTS])(shard_keys)
    slot_ids = jnp.arange(SLOTS, dtype=jnp.int32)
    marked = jnp.where(slot_ids[None, :] < counts[:, None], picks, SHARD)
    ordered = jnp.sort(marked, axis=1)
    return jnp.where(ordered < SHARD, ordered, 0).reshape(-1).astype(jnp.int32)


def draw_window_count(key, part):
    return window_plan(key)[0]


def draw_handed(key, part):
    return window_plan(key)[1]


def setup_inputs(seed: int = 0) -> dict:
    key_list = jax.random.split(jax.random.key(seed), 5)
    event_codes = draw_event_codes(jax.random.fold_in(key_list[4], 71), 0)
    window_ends = draw_window_ends(jax.random.fold_in(key_list[4], 71), 0)
    window_count = draw_window_count(jax.random.fold_in(key_list[4], 71), 0)
    handed = draw_handed(jax.random.fold_in(key_list[4], 71), 0)
    return {"event_codes": event_codes, "window_ends": window_ends, "window_count": window_count, "handed": handed}


def reference(event_codes, window_ends, window_count, handed):
    labels = jnp.arange(CODES, dtype=jnp.int32)
    shards = event_codes.reshape(NSHARDS, SHARD)

    def shard_total(own_codes):
        return jnp.sum((own_codes[:, None] == labels[None, :]).astype(jnp.float32), axis=0)

    totals = lax.map(shard_total, shards)
    offsets = jnp.cumsum(totals, axis=0) - totals
    earlier = jnp.concatenate([jnp.full((1, SHARD), -1, jnp.int32), shards[:-1]], axis=0)
    end_rows = window_ends.reshape(NSHARDS, SLOTS)
    shard_ids = jnp.arange(NSHARDS, dtype=jnp.int32)

    def one_shard(inputs):
        own_codes, prior_codes, end_row, offset, shard_id = inputs
        joined = jnp.concatenate([prior_codes, own_codes])
        cumulative = jnp.cumsum((joined[:, None] == labels[None, :]).astype(jnp.float32), axis=0)
        upper_tally = cumulative[SHARD + end_row]
        lower_tally = cumulative[SHARD + end_row - WINDOW]
        window_tally = upper_tally - lower_tally
        running = offset[None, :] + (upper_tally - cumulative[SHARD - 1][None, :])
        end_position = shard_id * SHARD + end_row
        length = jnp.minimum(WINDOW, end_position + 1).astype(jnp.float32)
        share_rows = CODES * window_tally / length[:, None]
        gap_rows = share_rows - CODES * running / (end_position + 1).astype(jnp.float32)[:, None]
        return share_rows, gap_rows

    shares, gaps = lax.map(one_shard, (shards, earlier, end_rows, offsets, shard_ids))
    within = jnp.arange(NSHARDS, dtype=jnp.int32) % GROUP
    received = jnp.where(within == 0, 0, jnp.roll(handed, 1))
    prior_count = jnp.roll(window_count, 1)
    row_ids = jnp.arange(CAP, dtype=jnp.int32)

    def place(shard_id):
        arrived = received[shard_id]
        kept_count = window_count[shard_id] - handed[shard_id]
        prior_slot = jnp.clip(prior_count[shard_id] - arrived + row_ids, 0, SLOTS - 1)
        own_slot = jnp.clip(row_ids - arrived, 0, SLOTS - 1)
        from_prior = (row_ids < arrived)[:, None]
        own_valid = ((row_ids >= arrived) & (row_ids - arrived < kept_count))[:, None]
        previous = (shard_id + NSHARDS - 1) % NSHARDS

        def pick(table_rows):
            return jnp.where(from_prior, table_rows[previous][prior_slot],
                             jnp.where(own_valid, table_rows[shard_id][own_slot], 0.0))

        return pick(shares), pick(gaps)

    placed_share, placed_gap = lax.map(place, shard_ids)
    return placed_share.reshape(NSHARDS * CAP, CODES), placed_gap.reshape(NSHARDS * CAP, CODES)
```

```python
import functools

import jax
import jax.numpy as jnp
from jax import lax
from jax.experimental import pallas as pl
from jax.experimental.pallas import tpu as pltpu
from jax.sharding import PartitionSpec as P

CODES = 256
WINDOW = 4096
SHARD = 8192
CAP = 512
SLOTS = 768
HAND = CAP // 2
NY, NZ, NG = 4, 8, 8
PLANE = NY * NG
NSHARDS = NY * NZ * NG
LANES = 128
ROWS = SHARD // LANES
STEP = 1024
MESH = pl.DeviceIdType.MESH
NT = (((1,), (1,)), ((), ()))
F32 = jnp.float32
BF16 = jnp.bfloat16


def device_of(shard):
    return (shard // NG, shard % NG)


def one_hot(row):
    wide = jnp.broadcast_to(row.astype(F32), (16, LANES)).astype(BF16)
    wide = jnp.concatenate([wide] * (CODES // 16), axis=0)
    label = lax.broadcasted_iota(jnp.int32, (CODES, LANES), 0).astype(F32).astype(BF16)
    return jnp.where(wide == label, jnp.ones((), BF16), jnp.zeros((), BF16))


def one_hot_block(block):
    return jnp.concatenate([one_hot(block[i : i + 1]) for i in range(8)], axis=1)


def marks(ends, base, later):
    n = ends.shape[0]
    pieces = []
    for i in range(STEP // LANES):
        at = lax.broadcasted_iota(jnp.int32, (16, LANES), 1) + (base + i * LANES)
        at = jnp.concatenate([at.astype(jnp.int16)] * (n // 16), axis=0)
        hit = at > ends if later else at <= ends
        pieces.append(jnp.where(hit, jnp.ones((), BF16), jnp.zeros((), BF16)))
    return jnp.concatenate(pieces, axis=1)


def end_rows(note, first, n):
    line = jnp.concatenate([note[i : i + 1] for i in range(SLOTS // LANES)], axis=1)
    high = (line >> 8).astype(F32)
    low = (line & 255).astype(F32)
    both = jnp.concatenate(
        [jnp.broadcast_to(high, (LANES, SLOTS)), jnp.broadcast_to(low, (LANES, SLOTS))], axis=0
    ).astype(BF16)
    slot = lax.broadcasted_iota(jnp.int32, (n, SLOTS), 1)
    row = lax.broadcasted_iota(jnp.int32, (n, SLOTS), 0)
    pick = jnp.where(slot == row + first, 1.0, 0.0).astype(BF16)
    got = lax.dot_general(pick, both, NT, preferred_element_type=F32)
    return (got[:, :LANES] * 256.0 + got[:, LANES:]).astype(jnp.int32)


def dot_nt(a, b):
    return lax.dot_general(a, b, NT, preferred_element_type=F32)


def tally_kernel(
    codes_hbm, ends_hbm, count_ref, handed_ref,
    share_ref, run_ref, inv_ref, off_ref, arr_ref,
    own, prev, prior, note, got, mine, plane, sums, column, own_acc, tail_acc, got_acc,
    load_sem, p1_send, p1_recv, p2_send, p2_recv, pass_send, pass_recv,
):
    seq, grp = lax.axis_index("seq"), lax.axis_index("grp")
    y, z = seq // NZ, seq % NZ
    shard = seq * NG + grp
    spot = y * NG + grp

    load_codes = pltpu.make_async_copy(codes_hbm, own, load_sem.at[0])
    load_ends = pltpu.make_async_copy(ends_hbm, note.at[pl.ds(0, 6)], load_sem.at[1])
    load_codes.start()
    load_ends.start()

    barrier = pltpu.get_barrier_semaphore()

    def plane_peer(k):
        at = (spot + k) % PLANE
        return ((at // NG) * NZ + z, at % NG)

    def column_peer(k):
        return (y * NZ + (z + k) % NZ, grp)

    for k in range(1, PLANE):
        pl.semaphore_signal(barrier, inc=1, device_id=plane_peer(k), device_id_type=MESH)
    for k in range(1, NZ):
        pl.semaphore_signal(barrier, inc=1, device_id=column_peer(k), device_id_type=MESH)
    for back in (1, 2):
        @pl.when(shard >= back)
        def _():
            pl.semaphore_signal(barrier, inc=1, device_id=device_of(shard - back), device_id_type=MESH)

    note[6:7] = jnp.full((1, LANES), count_ref[0], jnp.int32)
    note[7:8] = jnp.full((1, LANES), handed_ref[0], jnp.int32)
    own_acc[...] = jnp.zeros_like(own_acc)
    tail_acc[...] = jnp.zeros_like(tail_acc)
    got_acc[...] = jnp.zeros_like(got_acc)

    load_codes.wait()

    def count_rows(i, total):
        block = own[pl.ds(pl.multiple_of(i * 8, 8), 8)]
        for j in range(8):
            total = total + one_hot(block[j : j + 1])
        return total

    spread = lax.fori_loop(0, ROWS // 8, count_rows, jnp.zeros((CODES, LANES), BF16))
    total = dot_nt(jnp.ones((8, LANES), BF16), spread)[0:1]
    mine[0] = total
    plane[spot] = total

    load_ends.wait()
    own_ends = end_rows(note[...], 0, CAP)
    ends16 = own_ends.astype(jnp.int16)
    starts16 = (own_ends - WINDOW).astype(jnp.int16)

    def first_half(i):
        codes = one_hot_block(own[pl.ds(pl.multiple_of(i * 8, 8), 8)])
        rows = jnp.concatenate([marks(ends16, i * STEP, False), marks(starts16, i * STEP, False)], axis=0)
        own_acc[...] += dot_nt(rows, codes)

    def second_half(i):
        codes = one_hot_block(own[pl.ds(pl.multiple_of(i * 8, 8), 8)])
        own_acc[pl.ds(0, CAP)] += dot_nt(marks(ends16, i * STEP, False), codes)

    pl.loop(0, 2)(first_half)

    pl.semaphore_wait(barrier, PLANE - 1 + NZ - 1 + jnp.minimum(NSHARDS - 1 - shard, 2))

    sends = []
    for k in range(1, PLANE):
        sends.append(pltpu.make_async_remote_copy(
            src_ref=mine.at[0], dst_ref=plane.at[spot], send_sem=p1_send.at[k], recv_sem=p1_recv.at[k],
            device_id=plane_peer(k), device_id_type=MESH))
    for send in sends:
        send.start()

    pass_codes = pltpu.make_async_remote_copy(
        src_ref=own, dst_ref=prev, send_sem=pass_send.at[0], recv_sem=pass_recv.at[0],
        device_id=device_of(jnp.minimum(shard + 1, NSHARDS - 1)), device_id_type=MESH)
    pass_note = pltpu.make_async_remote_copy(
        src_ref=note, dst_ref=got, send_sem=pass_send.at[1], recv_sem=pass_recv.at[1],
        device_id=device_of(jnp.minimum(shard + 1, NSHARDS - 1)), device_id_type=MESH)
    pass_tail = pltpu.make_async_remote_copy(
        src_ref=own.at[pl.ds(ROWS // 2, ROWS // 2)], dst_ref=prior, send_sem=pass_send.at[2], recv_sem=pass_recv.at[2],
        device_id=device_of(jnp.minimum(shard + 2, NSHARDS - 1)), device_id_type=MESH)

    @pl.when(shard + 1 < NSHARDS)
    def _():
        pass_note.start()
        pass_codes.start()

    @pl.when(shard + 2 < NSHARDS)
    def _():
        pass_tail.start()

    pl.loop(2, 4)(first_half)
    pl.loop(4, 8)(second_half)

    for send in sends:
        send.wait_recv()

    below = jnp.zeros((1, CODES), F32)
    level = jnp.zeros((1, CODES), F32)
    inside = jnp.zeros((1, CODES), F32)
    before = jnp.zeros((1, CODES), F32)
    for k in range(PLANE):
        part = plane[k]
        below = below + jnp.where(k // NG < y, part, 0.0)
        here = jnp.where(k // NG == y, part, 0.0)
        level = level + here
        inside = inside + jnp.where(k % NG < grp, here, 0.0)
        before = before + jnp.where(k % NG == grp - 1, here, 0.0)
    sums[0] = below
    sums[1] = below + level

    climbs = []
    for k in range(1, NZ):
        after = ((z + k) % NZ > z).astype(jnp.int32)
        climbs.append(pltpu.make_async_remote_copy(
            src_ref=sums.at[after], dst_ref=column.at[z], send_sem=p2_send.at[k], recv_sem=p2_recv.at[k],
            device_id=column_peer(k), device_id_type=MESH))
    for climb in climbs:
        climb.start()
    column[z] = below + inside

    @pl.when(shard >= 1)
    def _():
        pass_note.wait_recv()
        pass_codes.wait_recv()

    @pl.when(shard >= 2)
    def _():
        pass_tail.wait_recv()

    arrived = jnp.where(grp > 0, got[7:8], 0)
    arr_ref[...] = jnp.broadcast_to(arrived, (8, LANES))
    first = jnp.concatenate([got[6:7] - arrived] * (SLOTS // LANES), axis=1)
    got_ends = end_rows(got[...], first, HAND)
    gends16 = got_ends.astype(jnp.int16)
    gstarts16 = (got_ends - WINDOW).astype(jnp.int16)

    def prev_first(i):
        block = jnp.where(shard >= 1, prev[pl.ds(pl.multiple_of(i * 8, 8), 8)], -1)
        rows = jnp.concatenate([marks(gends16, i * STEP, False), marks(gstarts16, i * STEP, False)], axis=0)
        got_acc[pl.ds(0, 2 * HAND)] += dot_nt(rows, one_hot_block(block))

    def prev_second(i):
        block = jnp.where(shard >= 1, prev[pl.ds(pl.multiple_of(i * 8, 8), 8)], -1)
        rows = jnp.concatenate(
            [marks(gends16, i * STEP, False), marks(ends16, i * STEP - WINDOW, True)], axis=0)
        part = dot_nt(rows, one_hot_block(block))
        got_acc[pl.ds(0, HAND)] += part[:HAND]
        tail_acc[...] += part[HAND:]

    def prior_part(i):
        block = jnp.where(shard >= 2, prior[pl.ds(pl.multiple_of(i * 8, 8), 8)], -1)
        got_acc[pl.ds(2 * HAND, HAND)] += dot_nt(marks(gends16, i * STEP, True), one_hot_block(block))

    pl.loop(0, 4)(prev_first)
    pl.loop(4, 8)(prev_second)
    pl.loop(0, 4)(prior_part)

    def finish(at, n, ends, origin, held, window, earlier):
        upto = (ends + (origin * SHARD + 1)).astype(F32)
        inv = 256.0 / upto
        scale = 256.0 / jnp.minimum(upto, float(WINDOW))
        inv_ref[pl.ds(at, n)] = inv
        share_ref[pl.ds(at, n)] = window * jnp.concatenate([scale, scale], axis=1)
        run_ref[pl.ds(at, n)] = (held - earlier) * jnp.concatenate([inv, inv], axis=1)

    held = got_acc[pl.ds(0, HAND)]
    finish(0, HAND, got_ends, shard - 1, held,
           held - got_acc[pl.ds(HAND, HAND)] + got_acc[pl.ds(2 * HAND, HAND)], before)
    held = own_acc[pl.ds(0, CAP)]
    finish(HAND, CAP, own_ends, shard, held,
           held - own_acc[pl.ds(CAP, CAP)] + tail_acc[...], jnp.zeros((1, CODES), F32))

    for climb in climbs:
        climb.wait_recv()
    offset = column[0]
    for k in range(1, NZ):
        offset = offset + column[k]
    off_ref[...] = jnp.broadcast_to(offset, (8, CODES))

    for send in sends:
        send.wait_send()
    for climb in climbs:
        climb.wait_send()

    @pl.when(shard + 1 < NSHARDS)
    def _():
        pass_note.wait_send()
        pass_codes.wait_send()

    @pl.when(shard + 2 < NSHARDS)
    def _():
        pass_tail.wait_send()


def place_kernel(
    count_ref, handed_ref, share_ref, run_ref, inv_ref, off_ref, arr_ref,
    share_hbm, gap_hbm, share_buf, gap_buf, sem,
):
    arrived = jnp.max(arr_ref[0:1, 0:1])
    kept = count_ref[0] - handed_ref[0]
    offset = off_ref[0:1]
    n = LANES
    copies = []
    for i in range(CAP // n):
        row = lax.broadcasted_iota(jnp.int32, (n, CODES), 0) + i * n
        start = HAND + i * n - arrived
        whole = jnp.minimum(start // 8 * 8, HAND + CAP - n - 8)
        rest = start - whole

        def rows_at(begin, n):
            inv = inv_ref[pl.ds(begin, n)]
            share = share_ref[pl.ds(begin, n)]
            run = run_ref[pl.ds(begin, n)] + jnp.concatenate([inv, inv], axis=1) * offset
            return share, share - run

        share, gap = rows_at(pl.multiple_of(whole, 8), n + 8)
        share = pltpu.roll(share, n + 8 - rest, 0)[:n]
        gap = pltpu.roll(gap, n + 8 - rest, 0)[:n]
        valid = row - arrived < kept
        share = jnp.where(valid, share, 0.0)
        gap = jnp.where(valid, gap, 0.0)
        if i * n < HAND:
            early_share, early_gap = rows_at(i * n, n)
            share = jnp.where(row < arrived, early_share, share)
            gap = jnp.where(row < arrived, early_gap, gap)
        share_buf[pl.ds(i * n, n)] = share
        gap_buf[pl.ds(i * n, n)] = gap
        for j, (buf, out) in enumerate(((share_buf, share_hbm), (gap_buf, gap_hbm))):
            copy = pltpu.make_async_copy(buf.at[pl.ds(i * n, n)], out.at[pl.ds(i * n, n)], sem.at[j, i])
            copy.start()
            copies.append(copy)
    for copy in copies:
        copy.wait()


def local(event_codes, window_ends, window_count, handed):
    vmem = pl.BlockSpec(memory_space=pltpu.VMEM)
    smem = pl.BlockSpec(memory_space=pltpu.SMEM)
    hbm = pl.BlockSpec(memory_space=pl.ANY)
    far = pl.BlockSpec(memory_space=pltpu.HBM)
    total = HAND + CAP
    dma = pltpu.SemaphoreType.DMA
    tallies = pl.pallas_call(
        tally_kernel,
        out_shape=(
            jax.ShapeDtypeStruct((total, CODES), F32),
            jax.ShapeDtypeStruct((total, CODES), F32),
            jax.ShapeDtypeStruct((total, LANES), F32),
            jax.ShapeDtypeStruct((8, CODES), F32),
            jax.ShapeDtypeStruct((8, LANES), jnp.int32),
        ),
        in_specs=[far, far, smem, smem],
        out_specs=(vmem,) * 5,
        scratch_shapes=[
            pltpu.VMEM((ROWS, LANES), jnp.int32),
            pltpu.VMEM((ROWS, LANES), jnp.int32),
            pltpu.VMEM((ROWS // 2, LANES), jnp.int32),
            pltpu.VMEM((8, LANES), jnp.int32),
            pltpu.VMEM((8, LANES), jnp.int32),
            pltpu.VMEM((1, 1, CODES), F32),
            pltpu.VMEM((PLANE, 1, CODES), F32),
            pltpu.VMEM((2, 1, CODES), F32),
            pltpu.VMEM((NZ, 1, CODES), F32),
            pltpu.VMEM((2 * CAP, CODES), F32),
            pltpu.VMEM((CAP, CODES), F32),
            pltpu.VMEM((3 * HAND, CODES), F32),
            dma((2,)), dma((PLANE,)), dma((PLANE,)), dma((NZ,)), dma((NZ,)), dma((3,)), dma((3,)),
        ],
        compiler_params=pltpu.CompilerParams(
            collective_id=0, has_side_effects=True, vmem_limit_bytes=32 * 2**20),
        name="tally",
    )(event_codes.reshape(ROWS, LANES), window_ends.reshape(SLOTS // LANES, LANES), window_count, handed)
    return pl.pallas_call(
        place_kernel,
        out_shape=(jax.ShapeDtypeStruct((CAP, CODES), F32),) * 2,
        in_specs=[smem, smem] + [vmem] * 5,
        out_specs=(hbm, hbm),
        scratch_shapes=[pltpu.VMEM((CAP, CODES), F32), pltpu.VMEM((CAP, CODES), F32), dma((2, CAP // LANES))],
        compiler_params=pltpu.CompilerParams(vmem_limit_bytes=16 * 2**20),
        name="place",
    )(window_count, handed, *tallies)


def solution(mesh):
    both = ("seq", "grp")
    return jax.shard_map(
        local,
        mesh=mesh,
        in_specs=(P(both), P(both), P(both), P(both)),
        out_specs=(P(both, None), P(both, None)),
        check_vma=False,
    )
```

```python
import functools

import jax
import jax.numpy as jnp
from jax import lax
from jax.experimental import pallas as pl
from jax.experimental.pallas import tpu as pltpu
from jax.sharding import PartitionSpec as P

CODES = 256
WINDOW = 4096
SHARD = 8192
CAP = 512
SLOTS = 768
HAND = CAP // 2
NY, NZ, NG = 4, 8, 8
PLANE = NY * NG
NSHARDS = NY * NZ * NG
LANES = 128
ROWS = SHARD // LANES
BLOCK = 16
HALF_BLOCKS = SHARD // BLOCK // 2
MESH = pl.DeviceIdType.MESH
NT = (((1,), (1,)), ((), ()))
F32 = jnp.float32
BF16 = jnp.bfloat16


def device_of(shard):
    return (shard // NG, shard % NG)


def one_hot(row):
    wide = jnp.broadcast_to(row, (16, LANES)).astype(BF16)
    wide = jnp.concatenate([wide] * (CODES // 16), axis=0)
    label = lax.broadcasted_iota(jnp.int32, (CODES, LANES), 0).astype(F32).astype(BF16)
    return jnp.where(wide == label, jnp.ones((), BF16), jnp.zeros((), BF16))


def by_block(half):
    half = half.astype(F32)
    turned = [half] + [pltpu.roll(half, LANES - 32 * k, 1) for k in (1, 2, 3)]
    return jnp.transpose(jnp.concatenate(turned, axis=0))[:32]


def block_counts(rows):
    total = one_hot(rows[0:1])
    for i in range(1, BLOCK):
        total = total + one_hot(rows[i : i + 1])
    return total


def block_column():
    at = lax.broadcasted_iota(jnp.int32, (HALF_BLOCKS, HAND), 0)
    return (8 * (at & 31) + ((at >> 5) & 3) * 2 + (at >> 7)).astype(jnp.int16)


def tall(row, n):
    wide = jnp.broadcast_to(row, (16, row.shape[1])).astype(jnp.int16)
    return jnp.concatenate([wide] * (n // 16), axis=0)


def flag(hit):
    return jnp.where(hit, jnp.ones((), BF16), jnp.zeros((), BF16))


def ends_line(note, slots, base):
    line = jnp.concatenate([note[i : i + 1] for i in range(slots // LANES)], axis=1)
    high = jnp.broadcast_to((line >> 8) + base, (8, slots))
    low = jnp.broadcast_to(line & 255, (8, slots))
    row = lax.broadcasted_iota(jnp.int32, (8, slots), 0)
    return jnp.where(row == 0, high, low).astype(F32).astype(BF16)


def picks(slots, first, at):
    slot = lax.broadcasted_iota(jnp.int32, (slots, HAND), 0)
    lane = lax.broadcasted_iota(jnp.int32, (slots, HAND), 1)
    return flag((slot - lane - at).astype(jnp.int16) == tall(first, slots))


def dot(a, b):
    return jnp.dot(a, b, preferred_element_type=F32)


def dot_nt(a, b):
    return lax.dot_general(a, b, NT, preferred_element_type=F32)


def tally_kernel(
    codes_hbm, ends_hbm, count_hbm, handed_hbm,
    share_ref, gap_ref, inv_ref, off_ref,
    own, prev, prior, note, got, mine, plane, sums, column, counts, blocks, scalars,
    load_sem, p1_send, p1_recv, p2_send, p2_recv, pass_send, pass_recv,
):
    seq, grp = lax.axis_index("seq"), lax.axis_index("grp")
    y, z = seq // NZ, seq % NZ
    shard = seq * NG + grp
    spot = y * NG + grp

    load_codes = pltpu.make_async_copy(codes_hbm, own, load_sem.at[0])
    load_ends = pltpu.make_async_copy(ends_hbm, note.at[pl.ds(0, 6)], load_sem.at[1])
    load_count = pltpu.make_async_copy(count_hbm, scalars.at[0], load_sem.at[2])
    load_handed = pltpu.make_async_copy(handed_hbm, scalars.at[1], load_sem.at[3])
    load_codes.start()
    load_ends.start()
    load_count.start()
    load_handed.start()

    barrier = pltpu.get_barrier_semaphore()

    def plane_device(dy, dg):
        return ((y + dy) * NZ + z, (grp + dg + NG) % NG)

    def column_device(k):
        return (y * NZ + (z + k + NZ) % NZ, grp)

    def climbs_to(k):
        return jnp.logical_or(y > 0, (z + k) % NZ > z)

    def climbs_from(k):
        return jnp.logical_or(y > 0, (z - k + NZ) % NZ < z)

    def greet(device):
        pl.semaphore_signal(barrier, inc=1, device_id=device, device_id_type=MESH)

    for dy in range(NY):
        @pl.when(y >= dy)
        def _():
            for dg in range(NG):
                if dy or dg:
                    greet(plane_device(-dy, -dg))
    for k in range(1, NZ):
        pl.when(climbs_from(k))(functools.partial(greet, column_device(-k)))
    for back in (1, 2):
        pl.when(shard >= back)(functools.partial(greet, device_of(shard - back)))

    def enter(half, codes):
        by = by_block(codes)
        first, second = block_counts(by[:BLOCK]), block_counts(by[BLOCK:])
        at = half * HALF_BLOCKS
        counts[:, at : at + LANES] = first
        counts[:, at + LANES : at + HALF_BLOCKS] = second
        blocks[:, at : at + LANES] = by[:BLOCK].astype(BF16)
        blocks[:, at + LANES : at + HALF_BLOCKS] = by[BLOCK:].astype(BF16)
        return first + second

    load_codes.wait()
    spread = enter(3, own[0:32]) + enter(4, own[32:64])
    total = dot_nt(jnp.ones((8, LANES), BF16), spread)[0:1]
    mine[0] = total
    plane[spot] = total

    load_ends.wait()
    load_count.wait()
    load_handed.wait()
    note[6:7] = jnp.full((1, LANES), scalars[0, 0], jnp.int32)
    note[7:8] = jnp.full((1, LANES), scalars[1, 0], jnp.int32)

    pl.semaphore_wait(
        barrier,
        NG * (NY - y) - 1 + jnp.where(y > 0, NZ - 1, NZ - 1 - z) + jnp.minimum(NSHARDS - 1 - shard, 2))

    spreads = []
    for dy in range(NY):
        for dg in range(NG):
            if dy or dg:
                spreads.append((dy, pltpu.make_async_remote_copy(
                    src_ref=mine.at[0], dst_ref=plane.at[spot],
                    send_sem=p1_send.at[dy * NG + dg], recv_sem=p1_recv.at[dy * NG + dg],
                    device_id=plane_device(dy, dg), device_id_type=MESH)))

    def plane_all(valid, act):
        for dy in range(NY):
            @pl.when(valid(dy))
            def _():
                for at, copy in spreads:
                    if at == dy:
                        act(copy)

    plane_all(lambda dy: y + dy < NY, lambda copy: copy.start())

    pass_codes = pltpu.make_async_remote_copy(
        src_ref=own, dst_ref=prev, send_sem=pass_send.at[0], recv_sem=pass_recv.at[0],
        device_id=device_of(jnp.minimum(shard + 1, NSHARDS - 1)), device_id_type=MESH)
    pass_note = pltpu.make_async_remote_copy(
        src_ref=note, dst_ref=got, send_sem=pass_send.at[1], recv_sem=pass_recv.at[1],
        device_id=device_of(jnp.minimum(shard + 1, NSHARDS - 1)), device_id_type=MESH)
    pass_tail = pltpu.make_async_remote_copy(
        src_ref=own.at[pl.ds(ROWS // 2, ROWS // 2)], dst_ref=prior, send_sem=pass_send.at[2], recv_sem=pass_recv.at[2],
        device_id=device_of(jnp.minimum(shard + 2, NSHARDS - 1)), device_id_type=MESH)

    @pl.when(shard + 1 < NSHARDS)
    def _():
        pass_note.start()
        pass_codes.start()

    @pl.when(shard + 2 < NSHARDS)
    def _():
        pass_tail.start()

    plane_all(lambda dy: y >= dy, lambda copy: copy.wait_recv())

    below = jnp.zeros((1, CODES), F32)
    level = jnp.zeros((1, CODES), F32)
    inside = jnp.zeros((1, CODES), F32)
    for k in range(PLANE):
        part = plane[k]
        below = below + jnp.where(k // NG < y, part, 0.0)
        here = jnp.where(k // NG == y, part, 0.0)
        level = level + here
        inside = inside + jnp.where(k % NG < grp, here, 0.0)
    sums[0] = below
    sums[1] = below + level

    climbs = []
    for k in range(1, NZ):
        after = ((z + k) % NZ > z).astype(jnp.int32)
        climbs.append(pltpu.make_async_remote_copy(
            src_ref=sums.at[after], dst_ref=column.at[z], send_sem=p2_send.at[k], recv_sem=p2_recv.at[k],
            device_id=column_device(k), device_id_type=MESH))
    for k, climb in enumerate(climbs, 1):
        pl.when(climbs_to(k))(climb.start)
    column[z] = below + inside

    @pl.when(shard >= 1)
    def _():
        pass_note.wait_recv()
        pass_codes.wait_recv()

    inner = grp > 0
    arrived = jnp.where(inner, got[7:8], 0)
    arrived = jnp.concatenate([arrived, arrived], axis=1)
    behind = jnp.concatenate([got[6:7], got[6:7]], axis=1) - arrived
    kept = note[6:7] - note[7:8]
    kept = jnp.concatenate([kept, kept], axis=1)
    own_line = ends_line(note[...], CAP, SHARD // 256)
    got_line = jnp.where(inner, ends_line(got[...], SLOTS, 0).astype(F32), 0.0).astype(BF16)
    lane = lax.broadcasted_iota(jnp.int32, (1, HAND), 1)
    block_of = block_column()

    known = jnp.where(shard >= 1, prev[...], -1)
    spread = enter(1, known[0:32]) + enter(2, known[32:64])
    before = dot_nt(jnp.ones((8, LANES), BF16), spread)[0:1]

    @pl.when(shard >= 2)
    def _():
        pass_tail.wait_recv()

    enter(0, jnp.where(shard >= 2, prior[...], -1))

    for part in range(2):
        ends = dot(own_line[:, : HAND * (part + 1)], picks(HAND * (part + 1), -arrived, HAND * part))
        if part == 0:
            ends = ends + dot(got_line, picks(SLOTS, behind, 0))
        ends = (ends[0:1] * 256.0 + ends[1:2]).astype(jnp.int32)
        valid = lane + HAND * part - arrived < kept
        upto = (ends + ((shard - 1) * SHARD + 1)).astype(F32)
        inv = jnp.where(valid, 256.0 / upto, 0.0)
        scale = jnp.where(valid, 256.0 / jnp.minimum(upto, float(WINDOW)), 0.0)
        key = ends // BLOCK
        halves = range(1 + 2 * part, 5)
        left, right = HALF_BLOCKS * halves[0], HALF_BLOCKS * 5
        less, same = [], []
        for half in halves:
            there = tall(key - HALF_BLOCKS * (half - 1), HALF_BLOCKS)
            less.append(flag(block_of < there))
            same.append(flag(block_of == there))
        less, same = jnp.concatenate(less, axis=0), jnp.concatenate(same, axis=0)
        upper = dot(counts[:, left:right], less)
        lower = dot(counts[:, left - HALF_BLOCKS : right - HALF_BLOCKS], less)
        tail = dot(counts[:, left - HALF_BLOCKS : left], jnp.ones((HALF_BLOCKS, LANES), BF16))
        found = jnp.concatenate(
            [blocks[:, left:right], blocks[:, left - HALF_BLOCKS : right - HALF_BLOCKS]], axis=0)
        found = dot(found, same)
        place = lax.broadcasted_iota(jnp.int32, (2 * BLOCK, HAND), 0) % BLOCK
        found = jnp.where(place <= ends % BLOCK, found, -1.0)
        for side in range(2):
            at = slice(side * LANES, (side + 1) * LANES)
            high = upper[:, at] + block_counts(found[:BLOCK, at]).astype(F32)
            low = lower[:, at] + block_counts(found[BLOCK:, at]).astype(F32)
            share = (high + tail - low) * scale[:, at]
            gap = share - high * inv[:, at]
            rows = pl.ds(HAND * part + LANES * side, LANES)
            share_ref[rows] = jnp.transpose(share)
            gap_ref[rows] = jnp.transpose(gap)
            inv_ref[rows] = jnp.transpose(jnp.broadcast_to(inv[:, at], (LANES, LANES)))

    for k, climb in enumerate(climbs, 1):
        pl.when(climbs_from(k))(climb.wait_recv)
    offset = jnp.zeros((1, CODES), F32)
    for k in range(NZ):
        used = jnp.logical_or(y > 0, k <= z)
        offset = offset + jnp.where(used, column[k], 0.0)
    off_ref[0:1] = offset - before
    off_ref[1:2] = offset

    plane_all(lambda dy: y + dy < NY, lambda copy: copy.wait_send())
    for k, climb in enumerate(climbs, 1):
        pl.when(climbs_to(k))(climb.wait_send)

    @pl.when(shard + 1 < NSHARDS)
    def _():
        pass_note.wait_send()
        pass_codes.wait_send()

    @pl.when(shard + 2 < NSHARDS)
    def _():
        pass_tail.wait_send()


def place_kernel(share_ref, gap_ref, inv_ref, off_ref, share_hbm, gap_hbm, buf, sem):
    share = pltpu.make_async_copy(share_ref, share_hbm, sem.at[0])
    share.start()
    n = LANES
    copies = [share]
    for i in range(CAP // n):
        at = pl.ds(i * n, n)
        inv = inv_ref[at]
        offset = off_ref[0:1] if i * n < HAND else off_ref[1:2]
        buf[at] = gap_ref[at] - jnp.concatenate([inv, inv], axis=1) * offset
        copies.append(pltpu.make_async_copy(buf.at[at], gap_hbm.at[at], sem.at[1 + i]))
        copies[-1].start()
    for copy in copies:
        copy.wait()


def local(event_codes, window_ends, window_count, handed):
    vmem = pl.BlockSpec(memory_space=pltpu.VMEM)
    hbm = pl.BlockSpec(memory_space=pl.ANY)
    far = pl.BlockSpec(memory_space=pltpu.HBM)
    dma = pltpu.SemaphoreType.DMA

    def stay(array):
        return pltpu.with_memory_space_constraint(array, pltpu.HBM)

    tallies = pl.pallas_call(
        tally_kernel,
        out_shape=(
            jax.ShapeDtypeStruct((CAP, CODES), F32),
            jax.ShapeDtypeStruct((CAP, CODES), F32),
            jax.ShapeDtypeStruct((CAP, LANES), F32),
            jax.ShapeDtypeStruct((8, CODES), F32),
        ),
        in_specs=[far] * 4,
        out_specs=(vmem,) * 4,
        scratch_shapes=[
            pltpu.VMEM((ROWS, LANES), jnp.int32),
            pltpu.VMEM((ROWS, LANES), jnp.int32),
            pltpu.VMEM((ROWS // 2, LANES), jnp.int32),
            pltpu.VMEM((8, LANES), jnp.int32),
            pltpu.VMEM((8, LANES), jnp.int32),
            pltpu.VMEM((1, 1, CODES), F32),
            pltpu.VMEM((PLANE, 1, CODES), F32),
            pltpu.VMEM((2, 1, CODES), F32),
            pltpu.VMEM((NZ, 1, CODES), F32),
            pltpu.VMEM((CODES, 5 * HALF_BLOCKS), BF16),
            pltpu.VMEM((BLOCK, 5 * HALF_BLOCKS), BF16),
            pltpu.SMEM((2, 1), jnp.int32),
            dma((4,)), dma((PLANE,)), dma((PLANE,)), dma((NZ,)), dma((NZ,)), dma((3,)), dma((3,)),
        ],
        compiler_params=pltpu.CompilerParams(
            collective_id=0, has_side_effects=True, vmem_limit_bytes=32 * 2**20),
        name="tally",
    )(stay(event_codes.reshape(ROWS, LANES)), stay(window_ends.reshape(SLOTS // LANES, LANES)), window_count, handed)
    return pl.pallas_call(
        place_kernel,
        out_shape=(jax.ShapeDtypeStruct((CAP, CODES), F32),) * 2,
        in_specs=[vmem] * 4,
        out_specs=(hbm, hbm),
        scratch_shapes=[pltpu.VMEM((CAP, CODES), F32), dma((1 + CAP // LANES,))],
        compiler_params=pltpu.CompilerParams(vmem_limit_bytes=16 * 2**20),
        name="place",
    )(*tallies)


def solution(mesh):
    both = ("seq", "grp")
    return jax.shard_map(
        local,
        mesh=mesh,
        in_specs=(P(both), P(both), P(both), P(both)),
        out_specs=(P(both, None), P(both, None)),
        check_vma=False,
    )
```

```python
import functools

import jax
import jax.numpy as jnp
from jax import lax
from jax.experimental import pallas as pl
from jax.experimental.pallas import tpu as pltpu
from jax.sharding import PartitionSpec as P

CODES = 256
WINDOW = 4096
SHARD = 8192
CAP = 512
SLOTS = 768
HAND = CAP // 2
NY, NZ, NG = 4, 8, 8
PLANE = NY * NG
HUB = 1
NSHARDS = NY * NZ * NG
LANES = 128
ROWS = SHARD // LANES
BLOCK = 16
HALF_BLOCKS = SHARD // BLOCK // 2
MESH = pl.DeviceIdType.MESH
NT = (((1,), (1,)), ((), ()))
F32 = jnp.float32
BF16 = jnp.bfloat16


def device_of(shard):
    return (lax.div(shard, NG), lax.rem(shard, NG))


def one_hot(row):
    wide = jnp.broadcast_to(row, (16, LANES)).astype(BF16)
    wide = jnp.concatenate([wide] * (CODES // 16), axis=0)
    label = lax.broadcasted_iota(jnp.int32, (CODES, LANES), 0).astype(F32).astype(BF16)
    return jnp.where(wide == label, jnp.ones((), BF16), jnp.zeros((), BF16))


def by_block(half):
    half = half.astype(F32)
    turned = [half] + [pltpu.roll(half, LANES - 32 * k, 1) for k in (1, 2, 3)]
    return jnp.transpose(jnp.concatenate(turned, axis=0))[:32]


def block_counts(rows):
    total = one_hot(rows[0:1])
    for i in range(1, BLOCK):
        total = total + one_hot(rows[i : i + 1])
    return total


def block_column():
    at = lax.broadcasted_iota(jnp.int32, (HALF_BLOCKS, HAND), 0)
    return (8 * (at & 31) + ((at >> 5) & 3) * 2 + (at >> 7)).astype(jnp.int16)


def tall(row, n):
    wide = jnp.broadcast_to(row, (16, row.shape[1])).astype(jnp.int16)
    return jnp.concatenate([wide] * (n // 16), axis=0)


def flag(hit):
    return jnp.where(hit, jnp.ones((), BF16), jnp.zeros((), BF16))


def ends_line(note, slots, base):
    line = jnp.concatenate([note[i : i + 1] for i in range(slots // LANES)], axis=1)
    high = jnp.broadcast_to((line >> 8) + base, (8, slots))
    low = jnp.broadcast_to(line & 255, (8, slots))
    row = lax.broadcasted_iota(jnp.int32, (8, slots), 0)
    return jnp.where(row == 0, high, low).astype(F32).astype(BF16)


def picks(slots, first, at):
    slot = lax.broadcasted_iota(jnp.int32, (slots, HAND), 0)
    lane = lax.broadcasted_iota(jnp.int32, (slots, HAND), 1)
    return flag((slot - lane - at).astype(jnp.int16) == tall(first, slots))


def dot(a, b):
    return jnp.dot(a, b, preferred_element_type=F32)


def dot_nt(a, b):
    return lax.dot_general(a, b, NT, preferred_element_type=F32)


def tally_kernel(
    codes_hbm, ends_hbm, handed_hbm,
    share_ref, gap_ref, inv_ref, off_ref,
    own, prev, prior, note, got, mine, plane, sums, column, counts, blocks, scalars,
    load_sem, p1_send, p1_recv, p2_send, p2_recv, pass_send, pass_recv,
):
    seq, grp = lax.axis_index("seq"), lax.axis_index("grp")
    y, z = lax.div(seq, NZ), lax.rem(seq, NZ)
    shard = seq * NG + grp
    spot = y * NG + grp
    hub = grp == HUB

    load_codes = pltpu.make_async_copy(codes_hbm, own, load_sem.at[0])
    load_ends = pltpu.make_async_copy(ends_hbm, note.at[pl.ds(0, 6)], load_sem.at[1])
    load_handed = pltpu.make_async_copy(handed_hbm, scalars, load_sem.at[2])
    load_codes.start()
    load_ends.start()
    load_handed.start()

    barrier = pltpu.get_barrier_semaphore()

    def greet(row, group):
        pl.semaphore_signal(barrier, inc=1, device_id=(row, group), device_id_type=MESH)

    def feeds(z2):
        return jnp.logical_or(z2 < z, jnp.logical_and(y > 0, z2 != z))

    def fed(z2):
        return jnp.logical_or(z2 > z, jnp.logical_and(y > 0, z2 != z))

    for g2 in range(NG):
        pl.when(grp != g2)(functools.partial(greet, seq, g2))
    for z2 in range(NZ):
        pl.when(feeds(z2))(functools.partial(greet, y * NZ + z2, HUB))

    @pl.when(hub)
    def _():
        for y2 in range(NY - 1):
            @pl.when(y2 < y)
            def _():
                for g2 in range(NG):
                    greet(y2 * NZ + z, g2)

    for back in (1, 2):
        pl.when(shard >= back)(functools.partial(greet, *device_of(shard - back)))

    def enter(half, codes):
        by = by_block(codes)
        first, second = block_counts(by[:BLOCK]), block_counts(by[BLOCK:])
        at = half * HALF_BLOCKS
        counts[:, at : at + LANES] = first
        counts[:, at + LANES : at + HALF_BLOCKS] = second
        blocks[:, at : at + LANES] = by[:BLOCK].astype(BF16)
        blocks[:, at + LANES : at + HALF_BLOCKS] = by[BLOCK:].astype(BF16)
        return first + second

    load_codes.wait()
    spread = enter(3, own[0:32]) + enter(4, own[32:64])
    total = dot_nt(jnp.ones((8, LANES), BF16), spread)[0:1]
    mine[0] = total
    plane[spot] = total

    load_ends.wait()
    load_handed.wait()
    slots = jnp.sum((note[0:6] > 0).astype(F32), axis=0, keepdims=True)
    slots = jnp.sum(slots, axis=1, keepdims=True) + (note[0:1, 0:1] == 0).astype(F32)
    note[6:7] = jnp.broadcast_to(slots.astype(jnp.int32), (1, LANES))
    note[7:8] = jnp.full((1, LANES), scalars[0], jnp.int32)

    columns = jnp.where(hub, NG * jnp.where(y > 0, NZ - 1, NZ - 1 - z), 0)
    pl.semaphore_wait(barrier, NG - 1 + NY - 1 - y + columns + jnp.minimum(NSHARDS - 1 - shard, 2))

    def spread_to(row, group, sem, source):
        return pltpu.make_async_remote_copy(
            src_ref=mine.at[0], dst_ref=plane.at[source], send_sem=p1_send.at[sem], recv_sem=p1_recv.at[source],
            device_id=(row, group), device_id_type=MESH)

    to_hubs = [(y2, spread_to(y2 * NZ + z, HUB, NG + y2, spot)) for y2 in range(1, NY)]
    to_mates = [(g2, spread_to(seq, g2, g2, spot)) for g2 in (HUB, 0, 2, 3, 4, 5, 6, 7)]
    for y2, copy in to_hubs:
        pl.when(y2 > y)(copy.start)
    for g2, copy in to_mates:
        pl.when(grp != g2)(copy.start)

    pass_codes = pltpu.make_async_remote_copy(
        src_ref=own, dst_ref=prev, send_sem=pass_send.at[0], recv_sem=pass_recv.at[0],
        device_id=device_of(jnp.minimum(shard + 1, NSHARDS - 1)), device_id_type=MESH)
    pass_note = pltpu.make_async_remote_copy(
        src_ref=note, dst_ref=got, send_sem=pass_send.at[1], recv_sem=pass_recv.at[1],
        device_id=device_of(jnp.minimum(shard + 1, NSHARDS - 1)), device_id_type=MESH)
    pass_tail = pltpu.make_async_remote_copy(
        src_ref=own.at[pl.ds(ROWS // 2, ROWS // 2)], dst_ref=prior, send_sem=pass_send.at[2], recv_sem=pass_recv.at[2],
        device_id=device_of(jnp.minimum(shard + 2, NSHARDS - 1)), device_id_type=MESH)

    @pl.when(shard + 1 < NSHARDS)
    def _():
        pass_note.start()
        pass_codes.start()

    @pl.when(shard + 2 < NSHARDS)
    def _():
        pass_tail.start()

    def hear_mates():
        for g2 in range(NG):
            pl.when(grp != g2)(spread_to(seq, g2, g2, y * NG + g2).wait_recv)

    climbs = []
    for z2 in range(NZ):
        for g2 in range(NG):
            climbs.append((z2, g2, pltpu.make_async_remote_copy(
                src_ref=sums.at[(z2 > z).astype(jnp.int32)], dst_ref=column.at[z],
                send_sem=p2_send.at[z2 * NG + g2], recv_sem=p2_recv.at[z],
                device_id=(y * NZ + z2, g2), device_id_type=MESH)))

    def climb_all(act):
        for z2 in range(NZ):
            @pl.when(fed(z2))
            def _():
                for at, g2, copy in climbs:
                    if at == z2:
                        act(copy)
            @pl.when(jnp.logical_and(z2 == z, y > 0))
            def _():
                for at, g2, copy in climbs:
                    if at == z2 and g2 != HUB:
                        act(copy)

    @pl.when(hub)
    def _():
        below = jnp.zeros((1, CODES), F32)
        level = jnp.zeros((1, CODES), F32)
        hear_mates()
        for g2 in range(NG):
            level = level + plane[y * NG + g2]
        for y2 in range(NY - 1):
            @pl.when(y2 < y)
            def _():
                for g2 in range(NG):
                    spread_to(seq, g2, g2, y2 * NG + g2).wait_recv()
            for g2 in range(NG):
                below = below + jnp.where(y2 < y, plane[y2 * NG + g2], 0.0)
        sums[0] = below
        sums[1] = below + level
        column[z] = below
        climb_all(lambda copy: copy.start())

    @pl.when(shard >= 1)
    def _():
        pass_note.wait_recv()
        pass_codes.wait_recv()

    inner = grp > 0
    arrived = jnp.where(inner, got[7:8], 0)
    arrived = jnp.concatenate([arrived, arrived], axis=1)
    behind = jnp.concatenate([got[6:7], got[6:7]], axis=1) - arrived
    kept = note[6:7] - note[7:8]
    kept = jnp.concatenate([kept, kept], axis=1)
    own_line = ends_line(note[...], CAP, SHARD // 256)
    got_line = jnp.where(inner, ends_line(got[...], SLOTS, 0).astype(F32), 0.0).astype(BF16)
    lane = lax.broadcasted_iota(jnp.int32, (1, HAND), 1)
    block_of = block_column()

    known = jnp.where(shard >= 1, prev[...], -1)
    spread = enter(1, known[0:32]) + enter(2, known[32:64])
    before = dot_nt(jnp.ones((8, LANES), BF16), spread)[0:1]

    @pl.when(shard >= 2)
    def _():
        pass_tail.wait_recv()

    enter(0, jnp.where(shard >= 2, prior[...], -1))

    for part in range(2):
        ends = dot(own_line[:, : HAND * (part + 1)], picks(HAND * (part + 1), -arrived, HAND * part))
        if part == 0:
            ends = ends + dot(got_line, picks(SLOTS, behind, 0))
        ends = (ends[0:1] * 256.0 + ends[1:2]).astype(jnp.int32)
        valid = lane + HAND * part - arrived < kept
        upto = (ends + ((shard - 1) * SHARD + 1)).astype(F32)
        inv = jnp.where(valid, 256.0 / upto, 0.0)
        scale = jnp.where(valid, 256.0 / jnp.minimum(upto, float(WINDOW)), 0.0)
        key = ends // BLOCK
        halves = range(1 + 2 * part, 5)
        left, right = HALF_BLOCKS * halves[0], HALF_BLOCKS * 5
        less, same = [], []
        for half in halves:
            there = tall(key - HALF_BLOCKS * (half - 1), HALF_BLOCKS)
            less.append(flag(block_of < there))
            same.append(flag(block_of == there))
        less, same = jnp.concatenate(less, axis=0), jnp.concatenate(same, axis=0)
        upper = dot(counts[:, left:right], less)
        lower = dot(counts[:, left - HALF_BLOCKS : right - HALF_BLOCKS], less)
        tail = dot(counts[:, left - HALF_BLOCKS : left], jnp.ones((HALF_BLOCKS, LANES), BF16))
        found = jnp.concatenate(
            [blocks[:, left:right], blocks[:, left - HALF_BLOCKS : right - HALF_BLOCKS]], axis=0)
        found = dot(found, same)
        place = lax.broadcasted_iota(jnp.int32, (2 * BLOCK, HAND), 0) % BLOCK
        found = jnp.where(place <= ends % BLOCK, found, -1.0)
        for side in range(2):
            at = slice(side * LANES, (side + 1) * LANES)
            high = upper[:, at] + block_counts(found[:BLOCK, at]).astype(F32)
            low = lower[:, at] + block_counts(found[BLOCK:, at]).astype(F32)
            share = (high + tail - low) * scale[:, at]
            gap = share - high * inv[:, at]
            rows = pl.ds(HAND * part + LANES * side, LANES)
            share_ref[rows] = jnp.transpose(share)
            gap_ref[rows] = jnp.transpose(gap)
            inv_ref[rows] = jnp.transpose(jnp.broadcast_to(inv[:, at], (LANES, LANES)))

    pl.when(jnp.logical_not(hub))(hear_mates)
    inside = jnp.zeros((1, CODES), F32)
    for g2 in range(NG - 1):
        inside = inside + jnp.where(g2 < grp, plane[y * NG + g2], 0.0)

    def hear_column(z2):
        pltpu.make_async_remote_copy(
            src_ref=sums.at[0], dst_ref=column.at[z2], send_sem=p2_send.at[z2], recv_sem=p2_recv.at[z2],
            device_id=(y * NZ + z2, HUB), device_id_type=MESH).wait_recv()

    offset = inside
    for z2 in range(NZ):
        pl.when(jnp.logical_or(feeds(z2), jnp.logical_and(jnp.logical_not(hub), jnp.logical_and(z2 == z, y > 0))))(
            functools.partial(hear_column, z2))
    for z2 in range(NZ):
        offset = offset + jnp.where(jnp.logical_or(z2 < z, y > 0), column[z2], 0.0)
    off_ref[0:1] = offset - before
    off_ref[1:2] = offset

    for y2, copy in to_hubs:
        pl.when(y2 > y)(copy.wait_send)
    for g2, copy in to_mates:
        pl.when(grp != g2)(copy.wait_send)
    pl.when(hub)(functools.partial(climb_all, lambda copy: copy.wait_send()))

    @pl.when(shard + 1 < NSHARDS)
    def _():
        pass_note.wait_send()
        pass_codes.wait_send()

    @pl.when(shard + 2 < NSHARDS)
    def _():
        pass_tail.wait_send()


def place_kernel(share_ref, gap_ref, inv_ref, off_ref, share_hbm, gap_hbm, buf, sem):
    share = pltpu.make_async_copy(share_ref, share_hbm, sem.at[0])
    share.start()
    n = LANES
    copies = [share]
    for i in range(CAP // n):
        at = pl.ds(i * n, n)
        inv = inv_ref[at]
        offset = off_ref[0:1] if i * n < HAND else off_ref[1:2]
        buf[at] = gap_ref[at] - jnp.concatenate([inv, inv], axis=1) * offset
        copies.append(pltpu.make_async_copy(buf.at[at], gap_hbm.at[at], sem.at[1 + i]))
        copies[-1].start()
    for copy in copies:
        copy.wait()


def local(event_codes, window_ends, window_count, handed):
    vmem = pl.BlockSpec(memory_space=pltpu.VMEM)
    hbm = pl.BlockSpec(memory_space=pl.ANY)
    far = pl.BlockSpec(memory_space=pltpu.HBM)
    dma = pltpu.SemaphoreType.DMA

    def stay(array):
        return pltpu.with_memory_space_constraint(array, pltpu.HBM)

    tallies = pl.pallas_call(
        tally_kernel,
        out_shape=(
            jax.ShapeDtypeStruct((CAP, CODES), F32),
            jax.ShapeDtypeStruct((CAP, CODES), F32),
            jax.ShapeDtypeStruct((CAP, LANES), F32),
            jax.ShapeDtypeStruct((8, CODES), F32),
        ),
        in_specs=[far] * 3,
        out_specs=(vmem,) * 4,
        scratch_shapes=[
            pltpu.VMEM((ROWS, LANES), jnp.int32),
            pltpu.VMEM((ROWS, LANES), jnp.int32),
            pltpu.VMEM((ROWS // 2, LANES), jnp.int32),
            pltpu.VMEM((8, LANES), jnp.int32),
            pltpu.VMEM((8, LANES), jnp.int32),
            pltpu.VMEM((1, 1, CODES), F32),
            pltpu.VMEM((PLANE, 1, CODES), F32),
            pltpu.VMEM((2, 1, CODES), F32),
            pltpu.VMEM((NZ, 1, CODES), F32),
            pltpu.VMEM((CODES, 5 * HALF_BLOCKS), BF16),
            pltpu.VMEM((BLOCK, 5 * HALF_BLOCKS), BF16),
            pltpu.SMEM((1,), jnp.int32),
            dma((3,)), dma((NG + NY,)), dma((PLANE,)), dma((NZ * NG,)), dma((NZ,)), dma((3,)), dma((3,)),
        ],
        compiler_params=pltpu.CompilerParams(
            collective_id=0, has_side_effects=True, vmem_limit_bytes=32 * 2**20),
        name="tally",
    )(stay(event_codes.reshape(ROWS, LANES)), stay(window_ends.reshape(SLOTS // LANES, LANES)), handed)
    return pl.pallas_call(
        place_kernel,
        out_shape=(jax.ShapeDtypeStruct((CAP, CODES), F32),) * 2,
        in_specs=[vmem] * 4,
        out_specs=(hbm, hbm),
        scratch_shapes=[pltpu.VMEM((CAP, CODES), F32), dma((1 + CAP // LANES,))],
        compiler_params=pltpu.CompilerParams(vmem_limit_bytes=16 * 2**20),
        name="place",
    )(*tallies)


def solution(mesh):
    both = ("seq", "grp")
    return jax.shard_map(
        local,
        mesh=mesh,
        in_specs=(P(both), P(both), P(both), P(both)),
        out_specs=(P(both, None), P(both, None)),
        check_vma=False,
    )
```

```python
import functools

import jax
import jax.numpy as jnp
from jax import lax
from jax.experimental import pallas as pl
from jax.experimental.pallas import tpu as pltpu
from jax.sharding import PartitionSpec as P

CODES = 256
WINDOW = 4096
SHARD = 8192
CAP = 512
SLOTS = 768
HAND = CAP // 2
NY, NZ, NG = 4, 8, 8
PLANE = NY * NG
HUB = 1
NSHARDS = NY * NZ * NG
LANES = 128
ROWS = SHARD // LANES
BLOCK = 16
HALF_BLOCKS = SHARD // BLOCK // 2
MESH = pl.DeviceIdType.MESH
NT = (((1,), (1,)), ((), ()))
F32 = jnp.float32
BF16 = jnp.bfloat16


def device_of(shard):
    return (lax.div(shard, NG), lax.rem(shard, NG))


def one_hot(row):
    wide = jnp.broadcast_to(row, (16, LANES)).astype(BF16)
    wide = jnp.concatenate([wide] * (CODES // 16), axis=0)
    label = lax.broadcasted_iota(jnp.int32, (CODES, LANES), 0).astype(F32).astype(BF16)
    return jnp.where(wide == label, jnp.ones((), BF16), jnp.zeros((), BF16))


def by_block(half):
    half = half.astype(F32)
    turned = [half] + [pltpu.roll(half, LANES - 32 * k, 1) for k in (1, 2, 3)]
    return jnp.transpose(jnp.concatenate(turned, axis=0))[:32]


def block_counts(rows):
    total = one_hot(rows[0:1])
    for i in range(1, BLOCK):
        total = total + one_hot(rows[i : i + 1])
    return total


def block_column():
    at = lax.broadcasted_iota(jnp.int32, (HALF_BLOCKS, HAND), 0)
    return (8 * (at & 31) + ((at >> 5) & 3) * 2 + (at >> 7)).astype(jnp.int16)


def tall(row, n):
    wide = jnp.broadcast_to(row, (16, row.shape[1])).astype(jnp.int16)
    return jnp.concatenate([wide] * (n // 16), axis=0)


def flag(hit):
    return jnp.where(hit, jnp.ones((), BF16), jnp.zeros((), BF16))


def ends_line(note, slots, base):
    line = jnp.concatenate([note[i : i + 1] for i in range(slots // LANES)], axis=1)
    high = jnp.broadcast_to((line >> 8) + base, (8, slots))
    low = jnp.broadcast_to(line & 255, (8, slots))
    row = lax.broadcasted_iota(jnp.int32, (8, slots), 0)
    return jnp.where(row == 0, high, low).astype(F32).astype(BF16)


def picks(slots, first, at):
    slot = lax.broadcasted_iota(jnp.int32, (slots, HAND), 0)
    lane = lax.broadcasted_iota(jnp.int32, (slots, HAND), 1)
    return flag((slot - lane - at).astype(jnp.int16) == tall(first, slots))


def dot(a, b):
    return jnp.dot(a, b, preferred_element_type=F32)


def dot_nt(a, b):
    return lax.dot_general(a, b, NT, preferred_element_type=F32)


def tally_kernel(
    codes_hbm, ends_hbm, handed_hbm,
    share_ref, gap_ref, inv_ref, off_ref,
    own, prev, prior, note, got, mine, plane, sums, column, counts, blocks, scalars,
    load_sem, p1_send, p1_recv, p2_send, p2_recv, pass_send, pass_recv,
):
    seq, grp = lax.axis_index("seq"), lax.axis_index("grp")
    y, z = lax.div(seq, NZ), lax.rem(seq, NZ)
    shard = seq * NG + grp
    spot = y * NG + grp
    hub = grp == HUB

    load_codes = [
        pltpu.make_async_copy(codes_hbm.at[pl.ds(i * BLOCK, BLOCK)], own.at[pl.ds(i * BLOCK, BLOCK)], load_sem.at[2 + i])
        for i in range(ROWS // BLOCK)]
    load_ends = pltpu.make_async_copy(ends_hbm, note.at[pl.ds(0, 6)], load_sem.at[0])
    load_handed = pltpu.make_async_copy(handed_hbm, scalars, load_sem.at[1])
    for load in load_codes:
        load.start()
    load_ends.start()
    load_handed.start()

    barrier = pltpu.get_barrier_semaphore()

    def greet(row, group):
        pl.semaphore_signal(barrier, inc=1, device_id=(row, group), device_id_type=MESH)

    def feeds(z2):
        return jnp.logical_or(z2 < z, jnp.logical_and(y > 0, z2 != z))

    def fed(z2):
        return jnp.logical_or(z2 > z, jnp.logical_and(y > 0, z2 != z))

    @pl.when(hub)
    def _():
        for y2 in range(NY - 1):
            @pl.when(y2 < y)
            def _():
                for g2 in range(NG):
                    greet(y2 * NZ + z, g2)

    for g2 in range(NG):
        pl.when(grp != g2)(functools.partial(greet, seq, g2))
    for z2 in range(NZ):
        pl.when(feeds(z2))(functools.partial(greet, y * NZ + z2, HUB))

    for back in (1, 2):
        pl.when(shard >= back)(functools.partial(greet, *device_of(shard - back)))

    def enter(half, codes):
        by = by_block(codes)
        first, second = block_counts(by[:BLOCK]), block_counts(by[BLOCK:])
        at = half * HALF_BLOCKS
        counts[:, at : at + LANES] = first
        counts[:, at + LANES : at + HALF_BLOCKS] = second
        blocks[:, at : at + LANES] = by[:BLOCK].astype(BF16)
        blocks[:, at + LANES : at + HALF_BLOCKS] = by[BLOCK:].astype(BF16)
        return first + second

    spread = jnp.zeros((CODES, LANES), BF16)
    for i, load in enumerate(load_codes):
        load.wait()
        spread = spread + block_counts(own[i * BLOCK : (i + 1) * BLOCK].astype(F32))
    total = dot_nt(jnp.ones((8, LANES), BF16), spread)[0:1]
    mine[0] = total
    plane[spot] = total

    load_ends.wait()
    load_handed.wait()
    slots = jnp.sum((note[0:6] > 0).astype(F32), axis=0, keepdims=True)
    slots = jnp.sum(slots, axis=1, keepdims=True) + (note[0:1, 0:1] == 0).astype(F32)
    note[6:7] = jnp.broadcast_to(slots.astype(jnp.int32), (1, LANES))
    note[7:8] = jnp.full((1, LANES), scalars[0], jnp.int32)

    columns = jnp.where(hub, NG * jnp.where(y > 0, NZ - 1, NZ - 1 - z), 0)
    pl.semaphore_wait(barrier, NG - 1 + NY - 1 - y + columns + jnp.minimum(NSHARDS - 1 - shard, 2))

    def spread_to(row, group, sem, batch):
        return pltpu.make_async_remote_copy(
            src_ref=mine.at[0], dst_ref=plane.at[spot], send_sem=p1_send.at[sem], recv_sem=p1_recv.at[batch],
            device_id=(row, group), device_id_type=MESH)

    def batch_of(n, send_sem, recv_sem):
        return pltpu.make_async_remote_copy(
            src_ref=plane.at[pl.ds(0, n)], dst_ref=plane.at[pl.ds(0, n)], send_sem=send_sem, recv_sem=recv_sem,
            device_id=(seq, grp), device_id_type=MESH)

    to_hubs = [(y2, spread_to(y2 * NZ + z, HUB, y2, y)) for y2 in range(1, NY)]
    to_mates = [(g2, spread_to(seq, g2, 0, NY)) for g2 in (HUB, 0, 2, 3, 4, 5, 6, 7)]
    for y2, copy in to_hubs:
        pl.when(y2 > y)(copy.start)
    for g2, copy in to_mates:
        pl.when(grp != g2)(copy.start)

    pass_codes = pltpu.make_async_remote_copy(
        src_ref=own, dst_ref=prev, send_sem=pass_send.at[0], recv_sem=pass_recv.at[0],
        device_id=device_of(jnp.minimum(shard + 1, NSHARDS - 1)), device_id_type=MESH)
    pass_note = pltpu.make_async_remote_copy(
        src_ref=note, dst_ref=got, send_sem=pass_send.at[1], recv_sem=pass_recv.at[1],
        device_id=device_of(jnp.minimum(shard + 1, NSHARDS - 1)), device_id_type=MESH)
    pass_tail = pltpu.make_async_remote_copy(
        src_ref=own.at[pl.ds(ROWS // 2, ROWS // 2)], dst_ref=prior, send_sem=pass_send.at[2], recv_sem=pass_recv.at[2],
        device_id=device_of(jnp.minimum(shard + 2, NSHARDS - 1)), device_id_type=MESH)

    @pl.when(shard + 1 < NSHARDS)
    def _():
        pass_note.start()
        pass_codes.start()

    @pl.when(shard + 2 < NSHARDS)
    def _():
        pass_tail.start()

    enter(3, own[0:32])
    enter(4, own[32:64])

    def hear_mates():
        batch_of(NG - 1, p1_send.at[0], p1_recv.at[NY]).wait_recv()

    climbs = []
    for z2 in range(NZ):
        for g2 in range(NG):
            climbs.append((z2, g2, pltpu.make_async_remote_copy(
                src_ref=sums.at[(z2 > z).astype(jnp.int32)], dst_ref=column.at[z],
                send_sem=p2_send.at[z2], recv_sem=p2_recv.at[z],
                device_id=(y * NZ + z2, g2), device_id_type=MESH)))

    def climb_all(act):
        for z2 in range(NZ):
            @pl.when(fed(z2))
            def _():
                for at, g2, copy in climbs:
                    if at == z2:
                        act(copy)
            @pl.when(jnp.logical_and(z2 == z, y > 0))
            def _():
                for at, g2, copy in climbs:
                    if at == z2 and g2 != HUB:
                        act(copy)

    @pl.when(hub)
    def _():
        below = jnp.zeros((1, CODES), F32)
        level = jnp.zeros((1, CODES), F32)
        hear_mates()
        for g2 in range(NG):
            level = level + plane[y * NG + g2]
        for y2 in range(NY - 1):
            @pl.when(y2 < y)
            def _():
                batch_of(NG, p1_send.at[0], p1_recv.at[y2]).wait_recv()
            for g2 in range(NG):
                below = below + jnp.where(y2 < y, plane[y2 * NG + g2], 0.0)
        sums[0] = below
        sums[1] = below + level
        column[z] = below
        climb_all(lambda copy: copy.start())

    @pl.when(shard >= 1)
    def _():
        pass_note.wait_recv()
        pass_codes.wait_recv()

    inner = grp > 0
    arrived = jnp.where(inner, got[7:8], 0)
    arrived = jnp.concatenate([arrived, arrived], axis=1)
    behind = jnp.concatenate([got[6:7], got[6:7]], axis=1) - arrived
    kept = note[6:7] - note[7:8]
    kept = jnp.concatenate([kept, kept], axis=1)
    own_line = ends_line(note[...], CAP, SHARD // 256)
    got_line = jnp.where(inner, ends_line(got[...], SLOTS, 0).astype(F32), 0.0).astype(BF16)
    lane = lax.broadcasted_iota(jnp.int32, (1, HAND), 1)
    block_of = block_column()

    known = jnp.where(shard >= 1, prev[...], -1)
    spread = enter(1, known[0:32]) + enter(2, known[32:64])
    before = dot_nt(jnp.ones((8, LANES), BF16), spread)[0:1]

    @pl.when(shard >= 2)
    def _():
        pass_tail.wait_recv()

    enter(0, jnp.where(shard >= 2, prior[...], -1))

    for part in range(2):
        ends = dot(own_line[:, : HAND * (part + 1)], picks(HAND * (part + 1), -arrived, HAND * part))
        if part == 0:
            ends = ends + dot(got_line, picks(SLOTS, behind, 0))
        ends = (ends[0:1] * 256.0 + ends[1:2]).astype(jnp.int32)
        valid = lane + HAND * part - arrived < kept
        upto = (ends + ((shard - 1) * SHARD + 1)).astype(F32)
        inv = jnp.where(valid, 256.0 / upto, 0.0)
        scale = jnp.where(valid, 256.0 / jnp.minimum(upto, float(WINDOW)), 0.0)
        key = ends // BLOCK
        halves = range(1 + 2 * part, 5)
        left, right = HALF_BLOCKS * halves[0], HALF_BLOCKS * 5
        less, same = [], []
        for half in halves:
            there = tall(key - HALF_BLOCKS * (half - 1), HALF_BLOCKS)
            less.append(flag(block_of < there))
            same.append(flag(block_of == there))
        less, same = jnp.concatenate(less, axis=0), jnp.concatenate(same, axis=0)
        upper = dot(counts[:, left:right], less)
        lower = dot(counts[:, left - HALF_BLOCKS : right - HALF_BLOCKS], less)
        tail = dot(counts[:, left - HALF_BLOCKS : left], jnp.ones((HALF_BLOCKS, LANES), BF16))
        found = jnp.concatenate(
            [blocks[:, left:right], blocks[:, left - HALF_BLOCKS : right - HALF_BLOCKS]], axis=0)
        found = dot(found, same)
        place = lax.broadcasted_iota(jnp.int32, (2 * BLOCK, HAND), 0) % BLOCK
        found = jnp.where(place <= ends % BLOCK, found, -1.0)
        for side in range(2):
            at = slice(side * LANES, (side + 1) * LANES)
            high = upper[:, at] + block_counts(found[:BLOCK, at]).astype(F32)
            low = lower[:, at] + block_counts(found[BLOCK:, at]).astype(F32)
            share = (high + tail - low) * scale[:, at]
            gap = share - high * inv[:, at]
            rows = pl.ds(HAND * part + LANES * side, LANES)
            share_ref[rows] = jnp.transpose(share)
            gap_ref[rows] = jnp.transpose(gap)
            inv_ref[rows] = jnp.transpose(jnp.broadcast_to(inv[:, at], (LANES, LANES)))

    pl.when(jnp.logical_not(hub))(hear_mates)
    inside = jnp.zeros((1, CODES), F32)
    for g2 in range(NG - 1):
        inside = inside + jnp.where(g2 < grp, plane[y * NG + g2], 0.0)

    for y2, copy in to_hubs:
        pl.when(y2 > y)(copy.wait_send)
    batch_of(NG - 1, p1_send.at[0], p1_recv.at[NY]).wait_send()

    @pl.when(hub)
    def _():
        for z2 in range(NZ):
            pl.when(fed(z2))(batch_of(NG, p2_send.at[z2], p1_recv.at[NY]).wait_send)
            pl.when(jnp.logical_and(z2 == z, y > 0))(batch_of(NG - 1, p2_send.at[z2], p1_recv.at[NY]).wait_send)

    @pl.when(shard + 1 < NSHARDS)
    def _():
        pass_note.wait_send()
        pass_codes.wait_send()

    @pl.when(shard + 2 < NSHARDS)
    def _():
        pass_tail.wait_send()

    def hear_column(z2):
        pltpu.make_async_remote_copy(
            src_ref=sums.at[0], dst_ref=column.at[z2], send_sem=p2_send.at[z2], recv_sem=p2_recv.at[z2],
            device_id=(y * NZ + z2, HUB), device_id_type=MESH).wait_recv()

    offset = inside
    for z2 in range(NZ):
        pl.when(jnp.logical_or(feeds(z2), jnp.logical_and(jnp.logical_not(hub), jnp.logical_and(z2 == z, y > 0))))(
            functools.partial(hear_column, z2))
    for z2 in range(NZ):
        offset = offset + jnp.where(jnp.logical_or(z2 < z, y > 0), column[z2], 0.0)
    off_ref[0:1] = offset - before
    off_ref[1:2] = offset


def place_kernel(share_ref, gap_ref, inv_ref, off_ref, share_hbm, gap_hbm, buf, sem):
    share = pltpu.make_async_copy(share_ref, share_hbm, sem.at[0])
    share.start()
    n = LANES
    copies = [share]
    for i in range(CAP // n):
        at = pl.ds(i * n, n)
        inv = inv_ref[at]
        offset = off_ref[0:1] if i * n < HAND else off_ref[1:2]
        buf[at] = gap_ref[at] - jnp.concatenate([inv, inv], axis=1) * offset
        copies.append(pltpu.make_async_copy(buf.at[at], gap_hbm.at[at], sem.at[1 + i]))
        copies[-1].start()
    for copy in copies:
        copy.wait()


def local(event_codes, window_ends, window_count, handed):
    vmem = pl.BlockSpec(memory_space=pltpu.VMEM)
    hbm = pl.BlockSpec(memory_space=pl.ANY)
    far = pl.BlockSpec(memory_space=pltpu.HBM)
    dma = pltpu.SemaphoreType.DMA

    def stay(array):
        return pltpu.with_memory_space_constraint(array, pltpu.HBM)

    tallies = pl.pallas_call(
        tally_kernel,
        out_shape=(
            jax.ShapeDtypeStruct((CAP, CODES), F32),
            jax.ShapeDtypeStruct((CAP, CODES), F32),
            jax.ShapeDtypeStruct((CAP, LANES), F32),
            jax.ShapeDtypeStruct((8, CODES), F32),
        ),
        in_specs=[far] * 3,
        out_specs=(vmem,) * 4,
        scratch_shapes=[
            pltpu.VMEM((ROWS, LANES), jnp.int32),
            pltpu.VMEM((ROWS, LANES), jnp.int32),
            pltpu.VMEM((ROWS // 2, LANES), jnp.int32),
            pltpu.VMEM((8, LANES), jnp.int32),
            pltpu.VMEM((8, LANES), jnp.int32),
            pltpu.VMEM((1, 1, CODES), F32),
            pltpu.VMEM((PLANE, 1, CODES), F32),
            pltpu.VMEM((2, 1, CODES), F32),
            pltpu.VMEM((NZ, 1, CODES), F32),
            pltpu.VMEM((CODES, 5 * HALF_BLOCKS), BF16),
            pltpu.VMEM((BLOCK, 5 * HALF_BLOCKS), BF16),
            pltpu.SMEM((1,), jnp.int32),
            dma((2 + ROWS // BLOCK,)), dma((NY,)), dma((NY + 1,)), dma((NZ,)), dma((NZ,)), dma((3,)), dma((3,)),
        ],
        compiler_params=pltpu.CompilerParams(
            collective_id=0, has_side_effects=True, vmem_limit_bytes=32 * 2**20),
        name="tally",
    )(stay(event_codes.reshape(ROWS, LANES)), stay(window_ends.reshape(SLOTS // LANES, LANES)), handed)
    return pl.pallas_call(
        place_kernel,
        out_shape=(jax.ShapeDtypeStruct((CAP, CODES), F32),) * 2,
        in_specs=[vmem] * 4,
        out_specs=(hbm, hbm),
        scratch_shapes=[pltpu.VMEM((CAP, CODES), F32), dma((1 + CAP // LANES,))],
        compiler_params=pltpu.CompilerParams(vmem_limit_bytes=16 * 2**20),
        name="place",
    )(*tallies)


def solution(mesh):
    both = ("seq", "grp")
    return jax.shard_map(
        local,
        mesh=mesh,
        in_specs=(P(both), P(both), P(both), P(both)),
        out_specs=(P(both, None), P(both, None)),
        check_vma=False,
    )
```

```python
import functools

import jax
import jax.numpy as jnp
from jax import lax
from jax.experimental import pallas as pl
from jax.experimental.pallas import tpu as pltpu
from jax.sharding import PartitionSpec as P

CODES = 256
WINDOW = 4096
SHARD = 8192
CAP = 512
SLOTS = 768
HAND = CAP // 2
NY, NZ, NG = 4, 8, 8
PLANE = NY * NG
HUB = 1
NSHARDS = NY * NZ * NG
LANES = 128
ROWS = SHARD // LANES
BLOCK = 16
PIECES = 1
HALF_BLOCKS = SHARD // BLOCK // 2
MESH = pl.DeviceIdType.MESH
NT = (((1,), (1,)), ((), ()))
F32 = jnp.float32
BF16 = jnp.bfloat16


def device_of(shard):
    return (lax.div(shard, NG), lax.rem(shard, NG))


def one_hot(row):
    wide = jnp.broadcast_to(row, (16, LANES)).astype(BF16)
    wide = jnp.concatenate([wide] * (CODES // 16), axis=0)
    label = lax.broadcasted_iota(jnp.int32, (CODES, LANES), 0).astype(F32).astype(BF16)
    return jnp.where(wide == label, jnp.ones((), BF16), jnp.zeros((), BF16))


def by_block(half):
    half = half.astype(F32)
    turned = [half] + [pltpu.roll(half, LANES - 32 * k, 1) for k in (1, 2, 3)]
    return jnp.transpose(jnp.concatenate(turned, axis=0))[:32]


def block_counts(rows):
    total = one_hot(rows[0:1])
    for i in range(1, BLOCK):
        total = total + one_hot(rows[i : i + 1])
    return total


def block_column():
    at = lax.broadcasted_iota(jnp.int32, (HALF_BLOCKS, HAND), 0)
    return (8 * (at & 31) + ((at >> 5) & 3) * 2 + (at >> 7)).astype(jnp.int16)


def tall(row, n):
    wide = jnp.broadcast_to(row, (16, row.shape[1])).astype(jnp.int16)
    return jnp.concatenate([wide] * (n // 16), axis=0)


def flag(hit):
    return jnp.where(hit, jnp.ones((), BF16), jnp.zeros((), BF16))


def ends_line(note, slots, base):
    line = jnp.concatenate([note[i : i + 1] for i in range(slots // LANES)], axis=1)
    high = jnp.broadcast_to((line >> 8) + base, (8, slots))
    low = jnp.broadcast_to(line & 255, (8, slots))
    row = lax.broadcasted_iota(jnp.int32, (8, slots), 0)
    return jnp.where(row == 0, high, low).astype(F32).astype(BF16)


def picks(slots, first, at):
    slot = lax.broadcasted_iota(jnp.int32, (slots, HAND), 0)
    lane = lax.broadcasted_iota(jnp.int32, (slots, HAND), 1)
    return flag((slot - lane - at).astype(jnp.int16) == tall(first, slots))


def dot(a, b):
    return jnp.dot(a, b, preferred_element_type=F32)


def dot_nt(a, b):
    return lax.dot_general(a, b, NT, preferred_element_type=F32)


def tally_kernel(
    codes_hbm, ends_hbm, handed_hbm,
    share_ref, gap_ref, inv_ref, off_ref,
    own, prev, prior, note, got, mine, plane, sums, column, counts, blocks, scalars,
    load_sem, p1_send, p1_recv, p2_send, p2_recv, pass_send, pass_recv,
):
    seq, grp = lax.axis_index("seq"), lax.axis_index("grp")
    y, z = lax.div(seq, NZ), lax.rem(seq, NZ)
    shard = seq * NG + grp
    spot = y * NG + grp
    hub = grp == HUB

    load_codes = [
        pltpu.make_async_copy(codes_hbm.at[pl.ds(i * BLOCK, BLOCK)], own.at[pl.ds(i * BLOCK, BLOCK)], load_sem.at[2 + i])
        for i in range(ROWS // BLOCK)]
    load_ends = pltpu.make_async_copy(ends_hbm, note.at[pl.ds(0, 6)], load_sem.at[0])
    load_handed = pltpu.make_async_copy(handed_hbm, scalars, load_sem.at[1])
    for load in load_codes:
        load.start()
    load_ends.start()
    load_handed.start()

    barrier = pltpu.get_barrier_semaphore()

    def greet(row, group):
        pl.semaphore_signal(barrier, inc=1, device_id=(row, group), device_id_type=MESH)

    def feeds(z2):
        return jnp.logical_or(z2 < z, jnp.logical_and(y > 0, z2 != z))

    @pl.when(hub)
    def _():
        for y2 in range(NY - 1):
            @pl.when(y2 < y)
            def _():
                for g2 in range(NG):
                    greet(y2 * NZ + z, g2)
        for g2 in range(NG):
            if g2 != HUB:
                greet(seq, g2)

    pl.when(jnp.logical_not(hub))(functools.partial(greet, seq, HUB))
    for z2 in range(NZ):
        pl.when(feeds(z2))(functools.partial(greet, y * NZ + z2, HUB))

    for back in (1, 2):
        pl.when(shard >= back)(functools.partial(greet, *device_of(shard - back)))

    def enter(half, codes):
        by = by_block(codes)
        first, second = block_counts(by[:BLOCK]), block_counts(by[BLOCK:])
        at = half * HALF_BLOCKS
        counts[:, at : at + LANES] = first
        counts[:, at + LANES : at + HALF_BLOCKS] = second
        blocks[:, at : at + LANES] = by[:BLOCK].astype(BF16)
        blocks[:, at + LANES : at + HALF_BLOCKS] = by[BLOCK:].astype(BF16)
        return first + second

    def write_note():
        load_ends.wait()
        load_handed.wait()
        slots = jnp.sum((note[0:6] > 0).astype(F32), axis=0, keepdims=True)
        slots = jnp.sum(slots, axis=1, keepdims=True) + (note[0:1, 0:1] == 0).astype(F32)
        note[6:7] = jnp.broadcast_to(slots.astype(jnp.int32), (1, LANES))
        note[7:8] = jnp.full((1, LANES), scalars[0], jnp.int32)

    spread = jnp.zeros((CODES, LANES), BF16)
    for i, load in enumerate(load_codes):
        load.wait()
        if i + 1 == len(load_codes):
            write_note()
        spread = spread + block_counts(own[i * BLOCK : (i + 1) * BLOCK].astype(F32))
    total = dot_nt(jnp.ones((8, LANES), BF16), spread)[0:1]
    mine[0] = total
    plane[spot] = total

    columns = jnp.where(hub, NG * jnp.where(y > 0, NZ - 1, NZ - 1 - z), 0)
    pl.semaphore_wait(barrier, jnp.where(hub, NG - 1 + NY - 1 - y, NY - y) + columns + jnp.minimum(NSHARDS - 1 - shard, 2))

    def spread_to(row, group, batch):
        return pltpu.make_async_remote_copy(
            src_ref=mine.at[0], dst_ref=plane.at[spot], send_sem=p1_send.at[0], recv_sem=p1_recv.at[batch],
            device_id=(row, group), device_id_type=MESH)

    def batch_of(n, send_sem, recv_sem):
        return pltpu.make_async_remote_copy(
            src_ref=plane.at[pl.ds(0, n)], dst_ref=plane.at[pl.ds(0, n)], send_sem=send_sem, recv_sem=recv_sem,
            device_id=(seq, grp), device_id_type=MESH)

    to_hubs = [(y2, spread_to(y2 * NZ + z, HUB, y)) for y2 in range(NY)]
    for y2, copy in to_hubs:
        pl.when(jnp.logical_or(y2 > y, jnp.logical_and(y2 == y, jnp.logical_not(hub))))(copy.start)

    pass_codes = pltpu.make_async_remote_copy(
        src_ref=own, dst_ref=prev, send_sem=pass_send.at[0], recv_sem=pass_recv.at[0],
        device_id=device_of(jnp.minimum(shard + 1, NSHARDS - 1)), device_id_type=MESH)
    pass_note = pltpu.make_async_remote_copy(
        src_ref=note, dst_ref=got, send_sem=pass_send.at[0], recv_sem=pass_recv.at[0],
        device_id=device_of(jnp.minimum(shard + 1, NSHARDS - 1)), device_id_type=MESH)
    pass_tail = pltpu.make_async_remote_copy(
        src_ref=own.at[pl.ds(ROWS // 2, ROWS // 2)], dst_ref=prior, send_sem=pass_send.at[0], recv_sem=pass_recv.at[1],
        device_id=device_of(jnp.minimum(shard + 2, NSHARDS - 1)), device_id_type=MESH)

    @pl.when(shard + 1 < NSHARDS)
    def _():
        pass_note.start()
        pass_codes.start()

    @pl.when(shard + 2 < NSHARDS)
    def _():
        pass_tail.start()

    enter(3, own[0:32])
    enter(4, own[32:64])

    def climb(z2, g2, kind):
        pltpu.make_async_remote_copy(
            src_ref=sums.at[kind], dst_ref=column.at[z], send_sem=p2_send.at[0], recv_sem=p2_recv.at[0],
            device_id=(y * NZ + z2, g2), device_id_type=MESH).start()

    @pl.when(hub)
    def _():
        sums[NG + 1] = jnp.zeros((1, CODES), F32)
        for y2 in range(NY - 1):
            @pl.when(y2 < y)
            def _():
                batch_of(NG, p1_send.at[0], p1_recv.at[y2]).wait_recv()
                part = sums[NG + 1]
                for g2 in range(NG):
                    part = part + plane[y2 * NG + g2]
                sums[NG + 1] = part
        for z2 in range(NZ - 1):
            @pl.when(jnp.logical_and(y > 0, z2 < z))
            def _():
                for g2 in range(NG):
                    climb(z2, g2, NG + 1)
        batch_of(NG - 1, p1_send.at[0], p1_recv.at[y]).wait_recv()
        below = sums[NG + 1]
        for g2 in range(NG):
            sums[g2] = below
            below = below + plane[y * NG + g2]
        sums[NG] = below
        for z2 in range(1, NZ):
            @pl.when(z2 > z)
            def _():
                for g2 in range(NG):
                    climb(z2, g2, NG)
        for g2 in range(NG):
            if g2 != HUB:
                climb(z, g2, g2)
        column[z] = sums[HUB]

    @pl.when(shard >= 1)
    def _():
        batch_of(4 + 32, p1_send.at[0], pass_recv.at[0]).wait_recv()

    inner = grp > 0
    arrived = jnp.where(inner, got[7:8], 0)
    arrived = jnp.concatenate([arrived, arrived], axis=1)
    behind = jnp.concatenate([got[6:7], got[6:7]], axis=1) - arrived
    kept = note[6:7] - note[7:8]
    kept = jnp.concatenate([kept, kept], axis=1)
    own_line = ends_line(note[...], CAP, SHARD // 256)
    got_line = jnp.where(inner, ends_line(got[...], SLOTS, 0).astype(F32), 0.0).astype(BF16)
    lane = lax.broadcasted_iota(jnp.int32, (1, HAND), 1)
    block_of = block_column()

    known = jnp.where(shard >= 1, prev[...], -1)
    spread = enter(1, known[0:32]) + enter(2, known[32:64])
    before = dot_nt(jnp.ones((8, LANES), BF16), spread)[0:1]

    @pl.when(shard >= 2)
    def _():
        pass_tail.wait_recv()

    enter(0, jnp.where(shard >= 2, prior[...], -1))

    for part in range(2):
        ends = dot(own_line[:, : HAND * (part + 1)], picks(HAND * (part + 1), -arrived, HAND * part))
        if part == 0:
            ends = ends + dot(got_line, picks(SLOTS, behind, 0))
        ends = (ends[0:1] * 256.0 + ends[1:2]).astype(jnp.int32)
        valid = lane + HAND * part - arrived < kept
        upto = (ends + ((shard - 1) * SHARD + 1)).astype(F32)
        inv = jnp.where(valid, 256.0 / upto, 0.0)
        scale = jnp.where(valid, 256.0 / jnp.minimum(upto, float(WINDOW)), 0.0)
        key = ends // BLOCK
        halves = range(1 + 2 * part, 5)
        left, right = HALF_BLOCKS * halves[0], HALF_BLOCKS * 5
        less, same = [], []
        for half in halves:
            there = tall(key - HALF_BLOCKS * (half - 1), HALF_BLOCKS)
            less.append(flag(block_of < there))
            same.append(flag(block_of == there))
        less, same = jnp.concatenate(less, axis=0), jnp.concatenate(same, axis=0)
        upper = dot(counts[:, left:right], less)
        lower = dot(counts[:, left - HALF_BLOCKS : right - HALF_BLOCKS], less)
        tail = dot(counts[:, left - HALF_BLOCKS : left], jnp.ones((HALF_BLOCKS, LANES), BF16))
        found = jnp.concatenate(
            [blocks[:, left:right], blocks[:, left - HALF_BLOCKS : right - HALF_BLOCKS]], axis=0)
        found = dot(found, same)
        place = lax.broadcasted_iota(jnp.int32, (2 * BLOCK, HAND), 0) % BLOCK
        found = jnp.where(place <= ends % BLOCK, found, -1.0)
        for side in range(2):
            at = slice(side * LANES, (side + 1) * LANES)
            high = upper[:, at] + block_counts(found[:BLOCK, at]).astype(F32)
            low = lower[:, at] + block_counts(found[BLOCK:, at]).astype(F32)
            share = (high + tail - low) * scale[:, at]
            gap = share - high * inv[:, at]
            rows = pl.ds(HAND * part + LANES * side, LANES)
            share_ref[rows] = jnp.transpose(share)
            gap_ref[rows] = jnp.transpose(gap)
            inv_ref[rows] = jnp.transpose(jnp.broadcast_to(inv[:, at], (LANES, LANES)))

    for row in range(NY):
        pl.when(jnp.logical_and(y == row, jnp.logical_not(hub)))(
            batch_of(NY - row, p1_send.at[0], p1_recv.at[0]).wait_send)
        if row < NY - 1:
            pl.when(jnp.logical_and(y == row, hub))(batch_of(NY - 1 - row, p1_send.at[0], p1_recv.at[0]).wait_send)

    @pl.when(jnp.logical_and(hub, y > 0))
    def _():
        batch_of(NG * NZ - 1, p2_send.at[0], p1_recv.at[0]).wait_send()

    for row in range(NZ):
        pl.when(jnp.logical_and(hub, jnp.logical_and(y == 0, z == row)))(
            batch_of(NG * (NZ - 1 - row) + NG - 1, p2_send.at[0], p1_recv.at[0]).wait_send)

    @pl.when(shard + 2 < NSHARDS)
    def _():
        batch_of(4 + 32 + 16, pass_send.at[0], p1_recv.at[0]).wait_send()

    @pl.when(shard + 2 == NSHARDS)
    def _():
        batch_of(4 + 32, pass_send.at[0], p1_recv.at[0]).wait_send()

    @pl.when(y > 0)
    def _():
        pl.when(hub)(batch_of(NZ - 1, p1_send.at[0], p2_recv.at[0]).wait_recv)
        pl.when(jnp.logical_not(hub))(batch_of(NZ, p1_send.at[0], p2_recv.at[0]).wait_recv)

    for row in range(NZ):
        first = jnp.logical_and(y == 0, z == row)
        pl.when(jnp.logical_and(first, jnp.logical_not(hub)))(
            batch_of(row + 1, p1_send.at[0], p2_recv.at[0]).wait_recv)
        if row:
            pl.when(jnp.logical_and(first, hub))(batch_of(row, p1_send.at[0], p2_recv.at[0]).wait_recv)

    offset = jnp.zeros((1, CODES), F32)
    for z2 in range(NZ):
        offset = offset + jnp.where(jnp.logical_or(z2 <= z, y > 0), column[z2], 0.0)
    off_ref[0:1] = offset - before
    off_ref[1:2] = offset


def place_kernel(share_ref, gap_ref, inv_ref, off_ref, share_hbm, gap_hbm, buf, sem):
    share = pltpu.make_async_copy(share_ref, share_hbm, sem.at[0])
    share.start()
    copies = [share]
    n = CAP // PIECES
    for i in range(PIECES):
        for k in range(i * n, (i + 1) * n, LANES):
            at = pl.ds(k, LANES)
            offset = off_ref[0:1] if k < HAND else off_ref[1:2]
            inv = inv_ref[at]
            buf[at] = gap_ref[at] - jnp.concatenate([inv, inv], axis=1) * offset
        at = pl.ds(i * n, n)
        copies.append(pltpu.make_async_copy(buf.at[at], gap_hbm.at[at], sem.at[1 + i]))
        copies[-1].start()
    for copy in copies:
        copy.wait()


def local(event_codes, window_ends, window_count, handed):
    vmem = pl.BlockSpec(memory_space=pltpu.VMEM)
    hbm = pl.BlockSpec(memory_space=pl.ANY)
    far = pl.BlockSpec(memory_space=pltpu.HBM)
    dma = pltpu.SemaphoreType.DMA

    def stay(array):
        return pltpu.with_memory_space_constraint(array, pltpu.HBM)

    tallies = pl.pallas_call(
        tally_kernel,
        out_shape=(
            jax.ShapeDtypeStruct((CAP, CODES), F32),
            jax.ShapeDtypeStruct((CAP, CODES), F32),
            jax.ShapeDtypeStruct((CAP, LANES), F32),
            jax.ShapeDtypeStruct((8, CODES), F32),
        ),
        in_specs=[far] * 3,
        out_specs=(vmem,) * 4,
        scratch_shapes=[
            pltpu.VMEM((ROWS, LANES), jnp.int32),
            pltpu.VMEM((ROWS, LANES), jnp.int32),
            pltpu.VMEM((ROWS // 2, LANES), jnp.int32),
            pltpu.VMEM((8, LANES), jnp.int32),
            pltpu.VMEM((8, LANES), jnp.int32),
            pltpu.VMEM((1, 1, CODES), F32),
            pltpu.VMEM((NZ * NG, 1, CODES), F32),
            pltpu.VMEM((NG + 2, 1, CODES), F32),
            pltpu.VMEM((NZ, 1, CODES), F32),
            pltpu.VMEM((CODES, 5 * HALF_BLOCKS), BF16),
            pltpu.VMEM((BLOCK, 5 * HALF_BLOCKS), BF16),
            pltpu.SMEM((1,), jnp.int32),
            dma((2 + ROWS // BLOCK,)), dma((1,)), dma((NY,)), dma((1,)), dma((1,)), dma((1,)), dma((2,)),
        ],
        compiler_params=pltpu.CompilerParams(
            collective_id=0, has_side_effects=True, vmem_limit_bytes=32 * 2**20),
        name="tally",
    )(stay(event_codes.reshape(ROWS, LANES)), stay(window_ends.reshape(SLOTS // LANES, LANES)), handed)
    return pl.pallas_call(
        place_kernel,
        out_shape=(jax.ShapeDtypeStruct((CAP, CODES), F32),) * 2,
        in_specs=[vmem] * 4,
        out_specs=(hbm, hbm),
        scratch_shapes=[pltpu.VMEM((CAP, CODES), F32), dma((1 + PIECES,))],
        compiler_params=pltpu.CompilerParams(vmem_limit_bytes=16 * 2**20),
        name="place",
    )(*tallies)


def solution(mesh):
    both = ("seq", "grp")
    return jax.shard_map(
        local,
        mesh=mesh,
        in_specs=(P(both), P(both), P(both), P(both)),
        out_specs=(P(both, None), P(both, None)),
        check_vma=False,
    )
```

```python
import functools

import jax
import jax.numpy as jnp
from jax import lax
from jax.experimental import pallas as pl
from jax.experimental.pallas import tpu as pltpu
from jax.sharding import PartitionSpec as P

CODES = 256
WINDOW = 4096
SHARD = 8192
CAP = 512
SLOTS = 768
HAND = CAP // 2
NY, NZ, NG = 4, 8, 8
PLANE = NY * NG
HUB = 1
NSHARDS = NY * NZ * NG
LANES = 128
ROWS = SHARD // LANES
BLOCK = 16
PIECES = 1
HALF_BLOCKS = SHARD // BLOCK // 2
MESH = pl.DeviceIdType.MESH
NT = (((1,), (1,)), ((), ()))
F32 = jnp.float32
BF16 = jnp.bfloat16


def device_of(shard):
    return (lax.div(shard, NG), lax.rem(shard, NG))


def one_hot(row):
    wide = jnp.broadcast_to(row, (16, LANES)).astype(BF16)
    wide = jnp.concatenate([wide] * (CODES // 16), axis=0)
    label = lax.broadcasted_iota(jnp.int32, (CODES, LANES), 0).astype(F32).astype(BF16)
    return jnp.where(wide == label, jnp.ones((), BF16), jnp.zeros((), BF16))


def by_block(half):
    half = half.astype(F32)
    turned = [half] + [pltpu.roll(half, LANES - 32 * k, 1) for k in (1, 2, 3)]
    return jnp.transpose(jnp.concatenate(turned, axis=0))[:32]


def block_counts(rows):
    total = one_hot(rows[0:1])
    for i in range(1, BLOCK):
        total = total + one_hot(rows[i : i + 1])
    return total


def block_column():
    at = lax.broadcasted_iota(jnp.int32, (HALF_BLOCKS, HAND), 0)
    return (8 * (at & 31) + ((at >> 5) & 3) * 2 + (at >> 7)).astype(jnp.int16)


def tall(row, n):
    wide = jnp.broadcast_to(row, (16, row.shape[1])).astype(jnp.int16)
    return jnp.concatenate([wide] * (n // 16), axis=0)


def flag(hit):
    return jnp.where(hit, jnp.ones((), BF16), jnp.zeros((), BF16))


def ends_line(note, slots, base):
    line = jnp.concatenate([note[i : i + 1] for i in range(slots // LANES)], axis=1)
    high = jnp.broadcast_to((line >> 8) + base, (8, slots))
    low = jnp.broadcast_to(line & 255, (8, slots))
    row = lax.broadcasted_iota(jnp.int32, (8, slots), 0)
    return jnp.where(row == 0, high, low).astype(F32).astype(BF16)


def picks(slots, first, at):
    slot = lax.broadcasted_iota(jnp.int32, (slots, HAND), 0)
    lane = lax.broadcasted_iota(jnp.int32, (slots, HAND), 1)
    return flag((slot - lane - at).astype(jnp.int16) == tall(first, slots))


def dot(a, b):
    return jnp.dot(a, b, preferred_element_type=F32)


def dot_nt(a, b):
    return lax.dot_general(a, b, NT, preferred_element_type=F32)


def tally_kernel(
    codes_hbm, ends_hbm, handed_hbm,
    share_ref, gap_ref, inv_ref, off_ref,
    own, prev, prior, note, got, mine, plane, sums, column, counts, blocks, scalars,
    load_sem, p1_send, p1_recv, p2_send, p2_recv, pass_send, pass_recv, ready, home,
):
    seq, grp = lax.axis_index("seq"), lax.axis_index("grp")
    y, z = lax.div(seq, NZ), lax.rem(seq, NZ)
    shard = seq * NG + grp
    spot = y * NG + grp
    hub = grp == HUB

    load_codes = [
        pltpu.make_async_copy(codes_hbm.at[pl.ds(i * BLOCK, BLOCK)], own.at[pl.ds(i * BLOCK, BLOCK)], load_sem.at[2 + i])
        for i in range(ROWS // BLOCK)]
    load_ends = pltpu.make_async_copy(ends_hbm, note.at[pl.ds(0, 6)], load_sem.at[0])
    load_handed = pltpu.make_async_copy(handed_hbm, scalars, load_sem.at[1])
    for load in load_codes:
        load.start()
    load_ends.start()
    load_handed.start()

    barrier = pltpu.get_barrier_semaphore()

    def greet(row, group):
        pl.semaphore_signal(barrier, inc=1, device_id=(row, group), device_id_type=MESH)

    @pl.when(hub)
    def _():
        for y2 in range(NY - 1):
            @pl.when(y2 < y)
            def _():
                for g2 in range(NG):
                    greet(y2 * NZ + z, g2)
        for g2 in range(NG):
            if g2 != HUB:
                greet(seq, g2)
        for z2 in range(1, NZ):
            @pl.when(z2 > z)
            def _():
                for g2 in range(NG):
                    greet(y * NZ + z2, g2)

    for z2 in range(1, NZ):
        pl.when(jnp.logical_and(y > 0, z2 > z))(functools.partial(greet, y * NZ + z2, HUB))

    for back in (1, 2):
        pl.when(shard >= back)(functools.partial(greet, *device_of(shard - back)))

    def enter(half, codes):
        by = by_block(codes)
        first, second = block_counts(by[:BLOCK]), block_counts(by[BLOCK:])
        at = half * HALF_BLOCKS
        counts[:, at : at + LANES] = first
        counts[:, at + LANES : at + HALF_BLOCKS] = second
        blocks[:, at : at + LANES] = by[:BLOCK].astype(BF16)
        blocks[:, at + LANES : at + HALF_BLOCKS] = by[BLOCK:].astype(BF16)
        return first + second

    def write_note():
        load_ends.wait()
        load_handed.wait()
        slots = jnp.sum((note[0:6] > 0).astype(F32), axis=0, keepdims=True)
        slots = jnp.sum(slots, axis=1, keepdims=True) + (note[0:1, 0:1] == 0).astype(F32)
        note[6:7] = jnp.broadcast_to(slots.astype(jnp.int32), (1, LANES))
        note[7:8] = jnp.full((1, LANES), scalars[0], jnp.int32)

    spread = jnp.zeros((CODES, LANES), BF16)
    for i, load in enumerate(load_codes):
        load.wait()
        if i + 1 == len(load_codes):
            write_note()
        spread = spread + block_counts(own[i * BLOCK : (i + 1) * BLOCK].astype(F32))
    total = dot_nt(jnp.ones((8, LANES), BF16), spread)[0:1]
    mine[0] = total
    plane[spot] = total

    hears = jnp.where(hub, NY - 1 - y + jnp.where(y > 0, NG * z, 0), NY - y)
    pl.semaphore_wait(barrier, hears + z + jnp.minimum(NSHARDS - 1 - shard, 2))

    def answer(sem, row):
        pl.semaphore_signal(sem, inc=1, device_id=(row, HUB), device_id_type=MESH)

    def spread_to(row, group, batch):
        return pltpu.make_async_remote_copy(
            src_ref=mine.at[0], dst_ref=plane.at[spot], send_sem=p1_send.at[0], recv_sem=p1_recv.at[batch],
            device_id=(row, group), device_id_type=MESH)

    def batch_of(n, send_sem, recv_sem):
        return pltpu.make_async_remote_copy(
            src_ref=plane.at[pl.ds(0, n)], dst_ref=plane.at[pl.ds(0, n)], send_sem=send_sem, recv_sem=recv_sem,
            device_id=(seq, grp), device_id_type=MESH)

    to_hubs = [(y2, spread_to(y2 * NZ + z, HUB, y)) for y2 in range(NY)]
    for y2, copy in to_hubs:
        pl.when(jnp.logical_or(y2 > y, jnp.logical_and(y2 == y, jnp.logical_not(hub))))(copy.start)

    pass_codes = pltpu.make_async_remote_copy(
        src_ref=own, dst_ref=prev, send_sem=pass_send.at[0], recv_sem=pass_recv.at[0],
        device_id=device_of(jnp.minimum(shard + 1, NSHARDS - 1)), device_id_type=MESH)
    pass_note = pltpu.make_async_remote_copy(
        src_ref=note, dst_ref=got, send_sem=pass_send.at[0], recv_sem=pass_recv.at[0],
        device_id=device_of(jnp.minimum(shard + 1, NSHARDS - 1)), device_id_type=MESH)
    pass_tail = pltpu.make_async_remote_copy(
        src_ref=own.at[pl.ds(ROWS // 2, ROWS // 2)], dst_ref=prior, send_sem=pass_send.at[0], recv_sem=pass_recv.at[1],
        device_id=device_of(jnp.minimum(shard + 2, NSHARDS - 1)), device_id_type=MESH)

    @pl.when(shard + 1 < NSHARDS)
    def _():
        pass_note.start()
        pass_codes.start()

    @pl.when(shard + 2 < NSHARDS)
    def _():
        pass_tail.start()

    for z2 in range(NZ - 1):
        pl.when(z2 < z)(functools.partial(answer, ready, y * NZ + z2))
    pl.when(jnp.logical_not(hub))(functools.partial(answer, home, seq))

    enter(3, own[0:32])
    enter(4, own[32:64])

    def climb(z2, g2, kind):
        pltpu.make_async_remote_copy(
            src_ref=sums.at[kind], dst_ref=column.at[z], send_sem=p2_send.at[0], recv_sem=p2_recv.at[0],
            device_id=(y * NZ + z2, g2), device_id_type=MESH).start()

    def send_level():
        pl.semaphore_wait(ready, NG * (NZ - 1 - z))
        for z2 in range(1, NZ):
            @pl.when(z2 > z)
            def _():
                for g2 in range(NG):
                    climb(z2, g2, NG)

    @pl.when(hub)
    def _():
        sums[NG + 1] = jnp.zeros((1, CODES), F32)
        for y2 in range(NY - 1):
            @pl.when(y2 < y)
            def _():
                batch_of(NG, p1_send.at[0], p1_recv.at[y2]).wait_recv()
                part = sums[NG + 1]
                for g2 in range(NG):
                    part = part + plane[y2 * NG + g2]
                sums[NG + 1] = part
        for z2 in range(NZ - 1):
            @pl.when(jnp.logical_and(y > 0, z2 < z))
            def _():
                for g2 in range(NG):
                    climb(z2, g2, NG + 1)
        batch_of(NG - 1, p1_send.at[0], p1_recv.at[y]).wait_recv()
        below = sums[NG + 1]
        for g2 in range(NG):
            sums[g2] = below
            below = below + plane[y * NG + g2]
        sums[NG] = below
        pl.semaphore_wait(home, NG - 1)
        pl.when(jnp.logical_and(y > 0, z < NZ - 1))(send_level)
        for g2 in range(NG):
            if g2 != HUB:
                climb(z, g2, g2)
        column[z] = sums[HUB]

    @pl.when(shard >= 1)
    def _():
        batch_of(4 + 32, p1_send.at[0], pass_recv.at[0]).wait_recv()

    inner = grp > 0
    arrived = jnp.where(inner, got[7:8], 0)
    arrived = jnp.concatenate([arrived, arrived], axis=1)
    behind = jnp.concatenate([got[6:7], got[6:7]], axis=1) - arrived
    kept = note[6:7] - note[7:8]
    kept = jnp.concatenate([kept, kept], axis=1)
    own_line = ends_line(note[...], CAP, SHARD // 256)
    got_line = jnp.where(inner, ends_line(got[...], SLOTS, 0).astype(F32), 0.0).astype(BF16)
    lane = lax.broadcasted_iota(jnp.int32, (1, HAND), 1)
    block_of = block_column()

    known = jnp.where(shard >= 1, prev[...], -1)
    spread = enter(1, known[0:32]) + enter(2, known[32:64])
    before = dot_nt(jnp.ones((8, LANES), BF16), spread)[0:1]

    @pl.when(shard >= 2)
    def _():
        pass_tail.wait_recv()

    enter(0, jnp.where(shard >= 2, prior[...], -1))

    for part in range(2):
        ends = dot(own_line[:, : HAND * (part + 1)], picks(HAND * (part + 1), -arrived, HAND * part))
        if part == 0:
            ends = ends + dot(got_line, picks(SLOTS, behind, 0))
        ends = (ends[0:1] * 256.0 + ends[1:2]).astype(jnp.int32)
        valid = lane + HAND * part - arrived < kept
        upto = (ends + ((shard - 1) * SHARD + 1)).astype(F32)
        inv = jnp.where(valid, 256.0 / upto, 0.0)
        scale = jnp.where(valid, 256.0 / jnp.minimum(upto, float(WINDOW)), 0.0)
        key = ends // BLOCK
        halves = range(1 + 2 * part, 5)
        left, right = HALF_BLOCKS * halves[0], HALF_BLOCKS * 5
        less, same = [], []
        for half in halves:
            there = tall(key - HALF_BLOCKS * (half - 1), HALF_BLOCKS)
            less.append(flag(block_of < there))
            same.append(flag(block_of == there))
        less, same = jnp.concatenate(less, axis=0), jnp.concatenate(same, axis=0)
        upper = dot(counts[:, left:right], less)
        lower = dot(counts[:, left - HALF_BLOCKS : right - HALF_BLOCKS], less)
        tail = dot(counts[:, left - HALF_BLOCKS : left], jnp.ones((HALF_BLOCKS, LANES), BF16))
        found = jnp.concatenate(
            [blocks[:, left:right], blocks[:, left - HALF_BLOCKS : right - HALF_BLOCKS]], axis=0)
        found = dot(found, same)
        place = lax.broadcasted_iota(jnp.int32, (2 * BLOCK, HAND), 0) % BLOCK
        found = jnp.where(place <= ends % BLOCK, found, -1.0)
        for side in range(2):
            at = slice(side * LANES, (side + 1) * LANES)
            high = upper[:, at] + block_counts(found[:BLOCK, at]).astype(F32)
            low = lower[:, at] + block_counts(found[BLOCK:, at]).astype(F32)
            share = (high + tail - low) * scale[:, at]
            gap = share - high * inv[:, at]
            rows = pl.ds(HAND * part + LANES * side, LANES)
            share_ref[rows] = jnp.transpose(share)
            gap_ref[rows] = jnp.transpose(gap)
            inv_ref[rows] = jnp.transpose(jnp.broadcast_to(inv[:, at], (LANES, LANES)))

    pl.when(jnp.logical_and(hub, jnp.logical_and(y == 0, z < NZ - 1)))(send_level)

    for row in range(NY):
        pl.when(jnp.logical_and(y == row, jnp.logical_not(hub)))(
            batch_of(NY - row, p1_send.at[0], p1_recv.at[0]).wait_send)
        if row < NY - 1:
            pl.when(jnp.logical_and(y == row, hub))(batch_of(NY - 1 - row, p1_send.at[0], p1_recv.at[0]).wait_send)

    @pl.when(jnp.logical_and(hub, y > 0))
    def _():
        batch_of(NG * NZ - 1, p2_send.at[0], p1_recv.at[0]).wait_send()

    for row in range(NZ):
        pl.when(jnp.logical_and(hub, jnp.logical_and(y == 0, z == row)))(
            batch_of(NG * (NZ - 1 - row) + NG - 1, p2_send.at[0], p1_recv.at[0]).wait_send)

    @pl.when(shard + 2 < NSHARDS)
    def _():
        batch_of(4 + 32 + 16, pass_send.at[0], p1_recv.at[0]).wait_send()

    @pl.when(shard + 2 == NSHARDS)
    def _():
        batch_of(4 + 32, pass_send.at[0], p1_recv.at[0]).wait_send()

    @pl.when(y > 0)
    def _():
        pl.when(hub)(batch_of(NZ - 1, p1_send.at[0], p2_recv.at[0]).wait_recv)
        pl.when(jnp.logical_not(hub))(batch_of(NZ, p1_send.at[0], p2_recv.at[0]).wait_recv)

    for row in range(NZ):
        first = jnp.logical_and(y == 0, z == row)
        pl.when(jnp.logical_and(first, jnp.logical_not(hub)))(
            batch_of(row + 1, p1_send.at[0], p2_recv.at[0]).wait_recv)
        if row:
            pl.when(jnp.logical_and(first, hub))(batch_of(row, p1_send.at[0], p2_recv.at[0]).wait_recv)

    offset = jnp.zeros((1, CODES), F32)
    for z2 in range(NZ):
        offset = offset + jnp.where(jnp.logical_or(z2 <= z, y > 0), column[z2], 0.0)
    off_ref[0:1] = offset - before
    off_ref[1:2] = offset


def place_kernel(share_ref, gap_ref, inv_ref, off_ref, share_hbm, gap_hbm, buf, sem):
    share = pltpu.make_async_copy(share_ref, share_hbm, sem.at[0])
    share.start()
    copies = [share]
    n = CAP // PIECES
    for i in range(PIECES):
        for k in range(i * n, (i + 1) * n, LANES):
            at = pl.ds(k, LANES)
            offset = off_ref[0:1] if k < HAND else off_ref[1:2]
            inv = inv_ref[at]
            buf[at] = gap_ref[at] - jnp.concatenate([inv, inv], axis=1) * offset
        at = pl.ds(i * n, n)
        copies.append(pltpu.make_async_copy(buf.at[at], gap_hbm.at[at], sem.at[1 + i]))
        copies[-1].start()
    for copy in copies:
        copy.wait()


def local(event_codes, window_ends, window_count, handed):
    vmem = pl.BlockSpec(memory_space=pltpu.VMEM)
    hbm = pl.BlockSpec(memory_space=pl.ANY)
    far = pl.BlockSpec(memory_space=pltpu.HBM)
    dma = pltpu.SemaphoreType.DMA

    def stay(array):
        return pltpu.with_memory_space_constraint(array, pltpu.HBM)

    tallies = pl.pallas_call(
        tally_kernel,
        out_shape=(
            jax.ShapeDtypeStruct((CAP, CODES), F32),
            jax.ShapeDtypeStruct((CAP, CODES), F32),
            jax.ShapeDtypeStruct((CAP, LANES), F32),
            jax.ShapeDtypeStruct((8, CODES), F32),
        ),
        in_specs=[far] * 3,
        out_specs=(vmem,) * 4,
        scratch_shapes=[
            pltpu.VMEM((ROWS, LANES), jnp.int32),
            pltpu.VMEM((ROWS, LANES), jnp.int32),
            pltpu.VMEM((ROWS // 2, LANES), jnp.int32),
            pltpu.VMEM((8, LANES), jnp.int32),
            pltpu.VMEM((8, LANES), jnp.int32),
            pltpu.VMEM((1, 1, CODES), F32),
            pltpu.VMEM((NZ * NG, 1, CODES), F32),
            pltpu.VMEM((NG + 2, 1, CODES), F32),
            pltpu.VMEM((NZ, 1, CODES), F32),
            pltpu.VMEM((CODES, 5 * HALF_BLOCKS), BF16),
            pltpu.VMEM((BLOCK, 5 * HALF_BLOCKS), BF16),
            pltpu.SMEM((1,), jnp.int32),
            dma((2 + ROWS // BLOCK,)), dma((1,)), dma((NY,)), dma((1,)), dma((1,)), dma((1,)), dma((2,)),
            pltpu.SemaphoreType.REGULAR, pltpu.SemaphoreType.REGULAR,
        ],
        compiler_params=pltpu.CompilerParams(
            collective_id=0, has_side_effects=True, vmem_limit_bytes=32 * 2**20),
        name="tally",
    )(stay(event_codes.reshape(ROWS, LANES)), stay(window_ends.reshape(SLOTS // LANES, LANES)), handed)
    return pl.pallas_call(
        place_kernel,
        out_shape=(jax.ShapeDtypeStruct((CAP, CODES), F32),) * 2,
        in_specs=[vmem] * 4,
        out_specs=(hbm, hbm),
        scratch_shapes=[pltpu.VMEM((CAP, CODES), F32), dma((1 + PIECES,))],
        compiler_params=pltpu.CompilerParams(vmem_limit_bytes=16 * 2**20),
        name="place",
    )(*tallies)


def solution(mesh):
    both = ("seq", "grp")
    return jax.shard_map(
        local,
        mesh=mesh,
        in_specs=(P(both), P(both), P(both), P(both)),
        out_specs=(P(both, None), P(both, None)),
        check_vma=False,
    )
```

```python
import functools

import jax
import jax.numpy as jnp
from jax import lax
from jax.experimental import pallas as pl
from jax.experimental.pallas import tpu as pltpu
from jax.sharding import PartitionSpec as P

CODES = 256
WINDOW = 4096
SHARD = 8192
CAP = 512
SLOTS = 768
HAND = CAP // 2
NY, NZ, NG = 4, 8, 8
PLANE = NY * NG
HUB = 1
NSHARDS = NY * NZ * NG
LANES = 128
ROWS = SHARD // LANES
BLOCK = 16
PIECES = 1
HALF_BLOCKS = SHARD // BLOCK // 2
MESH = pl.DeviceIdType.MESH
NT = (((1,), (1,)), ((), ()))
F32 = jnp.float32
BF16 = jnp.bfloat16


def device_of(shard):
    return (lax.div(shard, NG), lax.rem(shard, NG))


def one_hot(row):
    wide = jnp.broadcast_to(row, (16, LANES)).astype(BF16)
    wide = jnp.concatenate([wide] * (CODES // 16), axis=0)
    label = lax.broadcasted_iota(jnp.int32, (CODES, LANES), 0).astype(F32).astype(BF16)
    return jnp.where(wide == label, jnp.ones((), BF16), jnp.zeros((), BF16))


def by_block(half):
    half = half.astype(F32)
    turned = [half] + [pltpu.roll(half, LANES - 32 * k, 1) for k in (1, 2, 3)]
    return jnp.transpose(jnp.concatenate(turned, axis=0))[:32]


def block_counts(rows):
    total = one_hot(rows[0:1])
    for i in range(1, BLOCK):
        total = total + one_hot(rows[i : i + 1])
    return total


def block_column():
    at = lax.broadcasted_iota(jnp.int32, (HALF_BLOCKS, HAND), 0)
    return (8 * (at & 31) + ((at >> 5) & 3) * 2 + (at >> 7)).astype(jnp.int16)


def tall(row, n):
    wide = jnp.broadcast_to(row, (16, row.shape[1])).astype(jnp.int16)
    return jnp.concatenate([wide] * (n // 16), axis=0)


def flag(hit):
    return jnp.where(hit, jnp.ones((), BF16), jnp.zeros((), BF16))


def ends_line(note, slots, base):
    line = jnp.concatenate([note[i : i + 1] for i in range(slots // LANES)], axis=1)
    high = jnp.broadcast_to((line >> 8) + base, (8, slots))
    low = jnp.broadcast_to(line & 255, (8, slots))
    row = lax.broadcasted_iota(jnp.int32, (8, slots), 0)
    return jnp.where(row == 0, high, low).astype(F32).astype(BF16)


def picks(slots, first, at):
    slot = lax.broadcasted_iota(jnp.int32, (slots, HAND), 0)
    lane = lax.broadcasted_iota(jnp.int32, (slots, HAND), 1)
    return flag((slot - lane - at).astype(jnp.int16) == tall(first, slots))


def dot(a, b):
    return jnp.dot(a, b, preferred_element_type=F32)


def dot_nt(a, b):
    return lax.dot_general(a, b, NT, preferred_element_type=F32)


def tally_kernel(
    codes_hbm, ends_hbm, handed_hbm,
    share_ref, gap_ref, inv_ref, off_ref,
    own, prev, prior, note, got, mine, plane, sums, column, counts, blocks, scalars,
    load_sem, p1_send, p1_recv, p2_send, p2_recv, pass_send, pass_recv, ready, home,
):
    seq, grp = lax.axis_index("seq"), lax.axis_index("grp")
    y, z = lax.div(seq, NZ), lax.rem(seq, NZ)
    shard = seq * NG + grp
    spot = y * NG + grp
    hub = grp == HUB

    load_codes = [
        pltpu.make_async_copy(codes_hbm.at[pl.ds(i * BLOCK, BLOCK)], own.at[pl.ds(i * BLOCK, BLOCK)], load_sem.at[2 + i])
        for i in range(ROWS // BLOCK)]
    load_ends = pltpu.make_async_copy(ends_hbm, note.at[pl.ds(0, 6)], load_sem.at[0])
    load_handed = pltpu.make_async_copy(handed_hbm, scalars, load_sem.at[1])
    for load in load_codes:
        load.start()
    load_ends.start()
    load_handed.start()

    barrier = pltpu.get_barrier_semaphore()

    def greet(row, group):
        pl.semaphore_signal(barrier, inc=1, device_id=(row, group), device_id_type=MESH)

    @pl.when(hub)
    def _():
        for y2 in range(NY - 1):
            @pl.when(y2 < y if y2 else y == 1)
            def _():
                for g2 in range(NG):
                    greet(y2 * NZ + z, g2)
        pl.when(y > 1)(functools.partial(greet, z, HUB))
        for g2 in range(NG):
            if g2 != HUB:
                greet(seq, g2)
        for z2 in range(1, NZ):
            @pl.when(z2 > z)
            def _():
                for g2 in range(NG):
                    greet(y * NZ + z2, g2)

    for z2 in range(1, NZ):
        pl.when(jnp.logical_and(y > 0, z2 > z))(functools.partial(greet, y * NZ + z2, HUB))

    for back in (1, 2):
        pl.when(shard >= back)(functools.partial(greet, *device_of(shard - back)))

    def enter(half, codes):
        by = by_block(codes)
        first, second = block_counts(by[:BLOCK]), block_counts(by[BLOCK:])
        at = half * HALF_BLOCKS
        counts[:, at : at + LANES] = first
        counts[:, at + LANES : at + HALF_BLOCKS] = second
        blocks[:, at : at + LANES] = by[:BLOCK].astype(BF16)
        blocks[:, at + LANES : at + HALF_BLOCKS] = by[BLOCK:].astype(BF16)
        return first + second

    def write_note():
        load_ends.wait()
        load_handed.wait()
        slots = jnp.sum((note[0:6] > 0).astype(F32), axis=0, keepdims=True)
        slots = jnp.sum(slots, axis=1, keepdims=True) + (note[0:1, 0:1] == 0).astype(F32)
        note[6:7] = jnp.broadcast_to(slots.astype(jnp.int32), (1, LANES))
        note[7:8] = jnp.full((1, LANES), scalars[0], jnp.int32)

    spread = jnp.zeros((CODES, LANES), BF16)
    for i, load in enumerate(load_codes):
        load.wait()
        if i + 1 == len(load_codes):
            write_note()
        spread = spread + block_counts(own[i * BLOCK : (i + 1) * BLOCK].astype(F32))
    total = dot_nt(jnp.ones((8, LANES), BF16), spread)[0:1]
    mine[0] = total
    plane[spot] = total

    hears = jnp.where(hub, NY - 1 - y + jnp.where(y > 0, NG * z, 0), jnp.where(y == 0, 2, NY - y))
    pl.semaphore_wait(barrier, hears + z + jnp.minimum(NSHARDS - 1 - shard, 2))

    def answer(sem, row):
        pl.semaphore_signal(sem, inc=1, device_id=(row, HUB), device_id_type=MESH)

    def spread_to(row, group, batch):
        return pltpu.make_async_remote_copy(
            src_ref=mine.at[0], dst_ref=plane.at[spot], send_sem=p1_send.at[0], recv_sem=p1_recv.at[batch],
            device_id=(row, group), device_id_type=MESH)

    def batch_of(n, send_sem, recv_sem):
        return pltpu.make_async_remote_copy(
            src_ref=plane.at[pl.ds(0, n)], dst_ref=plane.at[pl.ds(0, n)], send_sem=send_sem, recv_sem=recv_sem,
            device_id=(seq, grp), device_id_type=MESH)

    to_hubs = [(y2, spread_to(y2 * NZ + z, HUB, y)) for y2 in range(NY)]
    for y2, copy in to_hubs:
        later = jnp.logical_and(y2 > y, y > 0) if y2 > 1 else y2 > y
        pl.when(jnp.logical_or(later, jnp.logical_and(y2 == y, jnp.logical_not(hub))))(copy.start)

    pass_codes = pltpu.make_async_remote_copy(
        src_ref=own, dst_ref=prev, send_sem=pass_send.at[0], recv_sem=pass_recv.at[0],
        device_id=device_of(jnp.minimum(shard + 1, NSHARDS - 1)), device_id_type=MESH)
    pass_note = pltpu.make_async_remote_copy(
        src_ref=note, dst_ref=got, send_sem=pass_send.at[0], recv_sem=pass_recv.at[0],
        device_id=device_of(jnp.minimum(shard + 1, NSHARDS - 1)), device_id_type=MESH)
    pass_tail = pltpu.make_async_remote_copy(
        src_ref=own.at[pl.ds(ROWS // 2, ROWS // 2)], dst_ref=prior, send_sem=pass_send.at[0], recv_sem=pass_recv.at[1],
        device_id=device_of(jnp.minimum(shard + 2, NSHARDS - 1)), device_id_type=MESH)

    @pl.when(shard + 1 < NSHARDS)
    def _():
        pass_note.start()
        pass_codes.start()

    @pl.when(shard + 2 < NSHARDS)
    def _():
        pass_tail.start()

    for z2 in range(NZ - 1):
        pl.when(z2 < z)(functools.partial(answer, ready, y * NZ + z2))
    pl.when(jnp.logical_not(hub))(functools.partial(answer, home, seq))

    enter(3, own[0:32])
    enter(4, own[32:64])

    def climb(z2, g2, kind):
        pltpu.make_async_remote_copy(
            src_ref=sums.at[kind], dst_ref=column.at[z], send_sem=p2_send.at[0], recv_sem=p2_recv.at[0],
            device_id=(y * NZ + z2, g2), device_id_type=MESH).start()

    def send_level():
        pl.semaphore_wait(ready, NG * (NZ - 1 - z))
        for z2 in range(1, NZ):
            @pl.when(z2 > z)
            def _():
                for g2 in range(NG):
                    climb(z2, g2, NG)

    @pl.when(hub)
    def _():
        sums[NG + 1] = jnp.zeros((1, CODES), F32)
        @pl.when(y > 1)
        def _():
            batch_of(1, p1_send.at[0], p1_recv.at[0]).wait_recv()
            sums[NG + 1] = plane[0]

        for y2 in range(NY - 1):
            @pl.when(y2 < y if y2 else y == 1)
            def _():
                batch_of(NG, p1_send.at[0], p1_recv.at[y2]).wait_recv()
                part = sums[NG + 1]
                for g2 in range(NG):
                    part = part + plane[y2 * NG + g2]
                sums[NG + 1] = part
        for z2 in range(NZ - 1):
            @pl.when(jnp.logical_and(y > 0, z2 < z))
            def _():
                for g2 in range(NG):
                    climb(z2, g2, NG + 1)
        batch_of(NG - 1, p1_send.at[0], p1_recv.at[y]).wait_recv()
        below = sums[NG + 1]
        for g2 in range(NG):
            sums[g2] = below
            below = below + plane[y * NG + g2]
        sums[NG] = below

        @pl.when(y == 0)
        def _():
            for y2 in (2, 3):
                pltpu.make_async_remote_copy(
                    src_ref=sums.at[NG], dst_ref=plane.at[0], send_sem=p1_send.at[0], recv_sem=p1_recv.at[0],
                    device_id=(y2 * NZ + z, HUB), device_id_type=MESH).start()

        pl.semaphore_wait(home, NG - 1)
        pl.when(jnp.logical_and(y > 0, z < NZ - 1))(send_level)
        for g2 in range(NG):
            if g2 != HUB:
                climb(z, g2, g2)
        column[z] = sums[HUB]

    @pl.when(shard >= 1)
    def _():
        batch_of(4 + 32, p1_send.at[0], pass_recv.at[0]).wait_recv()

    inner = grp > 0
    arrived = jnp.where(inner, got[7:8], 0)
    arrived = jnp.concatenate([arrived, arrived], axis=1)
    behind = jnp.concatenate([got[6:7], got[6:7]], axis=1) - arrived
    kept = note[6:7] - note[7:8]
    kept = jnp.concatenate([kept, kept], axis=1)
    own_line = ends_line(note[...], CAP, SHARD // 256)
    got_line = jnp.where(inner, ends_line(got[...], SLOTS, 0).astype(F32), 0.0).astype(BF16)
    lane = lax.broadcasted_iota(jnp.int32, (1, HAND), 1)
    block_of = block_column()

    known = jnp.where(shard >= 1, prev[...], -1)
    spread = enter(1, known[0:32]) + enter(2, known[32:64])
    before = dot_nt(jnp.ones((8, LANES), BF16), spread)[0:1]

    @pl.when(shard >= 2)
    def _():
        pass_tail.wait_recv()

    enter(0, jnp.where(shard >= 2, prior[...], -1))

    for part in range(2):
        ends = dot(own_line[:, : HAND * (part + 1)], picks(HAND * (part + 1), -arrived, HAND * part))
        if part == 0:
            ends = ends + dot(got_line, picks(SLOTS, behind, 0))
        ends = (ends[0:1] * 256.0 + ends[1:2]).astype(jnp.int32)
        valid = lane + HAND * part - arrived < kept
        upto = (ends + ((shard - 1) * SHARD + 1)).astype(F32)
        inv = jnp.where(valid, 256.0 / upto, 0.0)
        scale = jnp.where(valid, 256.0 / jnp.minimum(upto, float(WINDOW)), 0.0)
        key = ends // BLOCK
        halves = range(1 + 2 * part, 5)
        left, right = HALF_BLOCKS * halves[0], HALF_BLOCKS * 5
        less, same = [], []
        for half in halves:
            there = tall(key - HALF_BLOCKS * (half - 1), HALF_BLOCKS)
            less.append(flag(block_of < there))
            same.append(flag(block_of == there))
        less, same = jnp.concatenate(less, axis=0), jnp.concatenate(same, axis=0)
        upper = dot(counts[:, left:right], less)
        lower = dot(counts[:, left - HALF_BLOCKS : right - HALF_BLOCKS], less)
        tail = dot(counts[:, left - HALF_BLOCKS : left], jnp.ones((HALF_BLOCKS, LANES), BF16))
        found = jnp.concatenate(
            [blocks[:, left:right], blocks[:, left - HALF_BLOCKS : right - HALF_BLOCKS]], axis=0)
        found = dot(found, same)
        place = lax.broadcasted_iota(jnp.int32, (2 * BLOCK, HAND), 0) % BLOCK
        found = jnp.where(place <= ends % BLOCK, found, -1.0)
        for side in range(2):
            at = slice(side * LANES, (side + 1) * LANES)
            high = upper[:, at] + block_counts(found[:BLOCK, at]).astype(F32)
            low = lower[:, at] + block_counts(found[BLOCK:, at]).astype(F32)
            share = (high + tail - low) * scale[:, at]
            gap = share - high * inv[:, at]
            rows = pl.ds(HAND * part + LANES * side, LANES)
            share_ref[rows] = jnp.transpose(share)
            gap_ref[rows] = jnp.transpose(gap)
            inv_ref[rows] = jnp.transpose(jnp.broadcast_to(inv[:, at], (LANES, LANES)))

    pl.when(jnp.logical_and(hub, jnp.logical_and(y == 0, z < NZ - 1)))(send_level)

    for row in range(NY):
        pl.when(jnp.logical_and(y == row, jnp.logical_not(hub)))(
            batch_of(NY - row if row else 2, p1_send.at[0], p1_recv.at[0]).wait_send)
        if row < NY - 1:
            pl.when(jnp.logical_and(y == row, hub))(batch_of(NY - 1 - row, p1_send.at[0], p1_recv.at[0]).wait_send)

    @pl.when(jnp.logical_and(hub, y > 0))
    def _():
        batch_of(NG * NZ - 1, p2_send.at[0], p1_recv.at[0]).wait_send()

    for row in range(NZ):
        pl.when(jnp.logical_and(hub, jnp.logical_and(y == 0, z == row)))(
            batch_of(NG * (NZ - 1 - row) + NG - 1, p2_send.at[0], p1_recv.at[0]).wait_send)

    @pl.when(shard + 2 < NSHARDS)
    def _():
        batch_of(4 + 32 + 16, pass_send.at[0], p1_recv.at[0]).wait_send()

    @pl.when(shard + 2 == NSHARDS)
    def _():
        batch_of(4 + 32, pass_send.at[0], p1_recv.at[0]).wait_send()

    @pl.when(y > 0)
    def _():
        pl.when(hub)(batch_of(NZ - 1, p1_send.at[0], p2_recv.at[0]).wait_recv)
        pl.when(jnp.logical_not(hub))(batch_of(NZ, p1_send.at[0], p2_recv.at[0]).wait_recv)

    for row in range(NZ):
        first = jnp.logical_and(y == 0, z == row)
        pl.when(jnp.logical_and(first, jnp.logical_not(hub)))(
            batch_of(row + 1, p1_send.at[0], p2_recv.at[0]).wait_recv)
        if row:
            pl.when(jnp.logical_and(first, hub))(batch_of(row, p1_send.at[0], p2_recv.at[0]).wait_recv)

    offset = jnp.zeros((1, CODES), F32)
    for z2 in range(NZ):
        offset = offset + jnp.where(jnp.logical_or(z2 <= z, y > 0), column[z2], 0.0)
    off_ref[0:1] = offset - before
    off_ref[1:2] = offset


def place_kernel(share_ref, gap_ref, inv_ref, off_ref, share_hbm, gap_hbm, buf, sem):
    share = pltpu.make_async_copy(share_ref, share_hbm, sem.at[0])
    share.start()
    copies = [share]
    n = CAP // PIECES
    for i in range(PIECES):
        for k in range(i * n, (i + 1) * n, LANES):
            at = pl.ds(k, LANES)
            offset = off_ref[0:1] if k < HAND else off_ref[1:2]
            inv = inv_ref[at]
            buf[at] = gap_ref[at] - jnp.concatenate([inv, inv], axis=1) * offset
        at = pl.ds(i * n, n)
        copies.append(pltpu.make_async_copy(buf.at[at], gap_hbm.at[at], sem.at[1 + i]))
        copies[-1].start()
    for copy in copies:
        copy.wait()


def local(event_codes, window_ends, window_count, handed):
    vmem = pl.BlockSpec(memory_space=pltpu.VMEM)
    hbm = pl.BlockSpec(memory_space=pl.ANY)
    far = pl.BlockSpec(memory_space=pltpu.HBM)
    dma = pltpu.SemaphoreType.DMA

    def stay(array):
        return pltpu.with_memory_space_constraint(array, pltpu.HBM)

    tallies = pl.pallas_call(
        tally_kernel,
        out_shape=(
            jax.ShapeDtypeStruct((CAP, CODES), F32),
            jax.ShapeDtypeStruct((CAP, CODES), F32),
            jax.ShapeDtypeStruct((CAP, LANES), F32),
            jax.ShapeDtypeStruct((8, CODES), F32),
        ),
        in_specs=[far] * 3,
        out_specs=(vmem,) * 4,
        scratch_shapes=[
            pltpu.VMEM((ROWS, LANES), jnp.int32),
            pltpu.VMEM((ROWS, LANES), jnp.int32),
            pltpu.VMEM((ROWS // 2, LANES), jnp.int32),
            pltpu.VMEM((8, LANES), jnp.int32),
            pltpu.VMEM((8, LANES), jnp.int32),
            pltpu.VMEM((1, 1, CODES), F32),
            pltpu.VMEM((NZ * NG, 1, CODES), F32),
            pltpu.VMEM((NG + 2, 1, CODES), F32),
            pltpu.VMEM((NZ, 1, CODES), F32),
            pltpu.VMEM((CODES, 5 * HALF_BLOCKS), BF16),
            pltpu.VMEM((BLOCK, 5 * HALF_BLOCKS), BF16),
            pltpu.SMEM((1,), jnp.int32),
            dma((2 + ROWS // BLOCK,)), dma((1,)), dma((NY,)), dma((1,)), dma((1,)), dma((1,)), dma((2,)),
            pltpu.SemaphoreType.REGULAR, pltpu.SemaphoreType.REGULAR,
        ],
        compiler_params=pltpu.CompilerParams(
            collective_id=0, has_side_effects=True, vmem_limit_bytes=32 * 2**20),
        name="tally",
    )(stay(event_codes.reshape(ROWS, LANES)), stay(window_ends.reshape(SLOTS // LANES, LANES)), handed)
    return pl.pallas_call(
        place_kernel,
        out_shape=(jax.ShapeDtypeStruct((CAP, CODES), F32),) * 2,
        in_specs=[vmem] * 4,
        out_specs=(hbm, hbm),
        scratch_shapes=[pltpu.VMEM((CAP, CODES), F32), dma((1 + PIECES,))],
        compiler_params=pltpu.CompilerParams(vmem_limit_bytes=16 * 2**20),
        name="place",
    )(*tallies)


def solution(mesh):
    both = ("seq", "grp")
    return jax.shard_map(
        local,
        mesh=mesh,
        in_specs=(P(both), P(both), P(both), P(both)),
        out_specs=(P(both, None), P(both, None)),
        check_vma=False,
    )
```

```python
import functools

import jax
import jax.numpy as jnp
from jax import lax
from jax.experimental import pallas as pl
from jax.experimental.pallas import tpu as pltpu
from jax.sharding import PartitionSpec as P

CODES = 256
WINDOW = 4096
SHARD = 8192
CAP = 512
SLOTS = 768
HAND = CAP // 2
NY, NZ, NG = 4, 8, 8
PLANE = NY * NG
HUB = 1
NSHARDS = NY * NZ * NG
LANES = 128
ROWS = SHARD // LANES
BLOCK = 16
PIECES = 1
HALF_BLOCKS = SHARD // BLOCK // 2
MESH = pl.DeviceIdType.MESH
NT = (((1,), (1,)), ((), ()))
F32 = jnp.float32
BF16 = jnp.bfloat16


def device_of(shard):
    return (lax.div(shard, NG), lax.rem(shard, NG))


def one_hot(row):
    wide = jnp.broadcast_to(row, (16, LANES)).astype(BF16)
    wide = jnp.concatenate([wide] * (CODES // 16), axis=0)
    label = lax.broadcasted_iota(jnp.int32, (CODES, LANES), 0).astype(F32).astype(BF16)
    return jnp.where(wide == label, jnp.ones((), BF16), jnp.zeros((), BF16))


def by_block(half):
    half = half.astype(F32)
    turned = [half] + [pltpu.roll(half, LANES - 32 * k, 1) for k in (1, 2, 3)]
    return jnp.transpose(jnp.concatenate(turned, axis=0))[:32]


def block_counts(rows):
    total = one_hot(rows[0:1])
    for i in range(1, BLOCK):
        total = total + one_hot(rows[i : i + 1])
    return total


def block_column():
    at = lax.broadcasted_iota(jnp.int32, (HALF_BLOCKS, HAND), 0)
    return (8 * (at & 31) + ((at >> 5) & 3) * 2 + (at >> 7)).astype(jnp.int16)


def tall(row, n):
    wide = jnp.broadcast_to(row, (16, row.shape[1])).astype(jnp.int16)
    return jnp.concatenate([wide] * (n // 16), axis=0)


def flag(hit):
    return jnp.where(hit, jnp.ones((), BF16), jnp.zeros((), BF16))


def ends_line(note, slots, base):
    line = jnp.concatenate([note[i : i + 1] for i in range(slots // LANES)], axis=1)
    high = jnp.broadcast_to((line >> 8) + base, (8, slots))
    low = jnp.broadcast_to(line & 255, (8, slots))
    row = lax.broadcasted_iota(jnp.int32, (8, slots), 0)
    return jnp.where(row == 0, high, low).astype(F32).astype(BF16)


def picks(slots, first, at):
    slot = lax.broadcasted_iota(jnp.int32, (slots, HAND), 0)
    lane = lax.broadcasted_iota(jnp.int32, (slots, HAND), 1)
    return flag((slot - lane - at).astype(jnp.int16) == tall(first, slots))


def dot(a, b):
    return jnp.dot(a, b, preferred_element_type=F32)


def dot_nt(a, b):
    return lax.dot_general(a, b, NT, preferred_element_type=F32)


def tally_kernel(
    codes_hbm, ends_hbm, handed_hbm,
    share_ref, gap_ref, inv_ref, off_ref,
    own, prev, prior, note, got, mine, plane, sums, column, counts, blocks, scalars,
    load_sem, p1_send, p1_recv, p2_send, p2_recv, pass_send, pass_recv, ready, home,
):
    seq, grp = lax.axis_index("seq"), lax.axis_index("grp")
    y, z = lax.div(seq, NZ), lax.rem(seq, NZ)
    shard = seq * NG + grp
    spot = y * NG + grp
    hub = grp == HUB

    load_codes = [
        pltpu.make_async_copy(codes_hbm.at[pl.ds(i * 32, 32)], own.at[pl.ds(i * 32, 32)], load_sem.at[2 + i])
        for i in range(ROWS // 32)]
    load_ends = pltpu.make_async_copy(ends_hbm, note.at[pl.ds(0, 6)], load_sem.at[0])
    load_handed = pltpu.make_async_copy(handed_hbm, scalars, load_sem.at[1])
    for load in load_codes:
        load.start()
    load_ends.start()
    load_handed.start()

    barrier = pltpu.get_barrier_semaphore()

    def greet(row, group):
        pl.semaphore_signal(barrier, inc=1, device_id=(row, group), device_id_type=MESH)

    @pl.when(hub)
    def _():
        for y2 in range(NY - 1):
            @pl.when(y2 < y)
            def _():
                for g2 in range(NG):
                    greet(y2 * NZ + z, g2)
        for g2 in range(NG):
            if g2 != HUB:
                greet(seq, g2)
        for z2 in range(1, NZ):
            @pl.when(z2 > z)
            def _():
                for g2 in range(NG):
                    greet(y * NZ + z2, g2)

    for z2 in range(1, NZ):
        pl.when(jnp.logical_and(y > 0, z2 > z))(functools.partial(greet, y * NZ + z2, HUB))

    for back in (1, 2):
        pl.when(shard >= back)(functools.partial(greet, *device_of(shard - back)))

    def enter(half, codes):
        by = by_block(codes)
        first, second = block_counts(by[:BLOCK]), block_counts(by[BLOCK:])
        at = half * HALF_BLOCKS
        counts[:, at : at + LANES] = first
        counts[:, at + LANES : at + HALF_BLOCKS] = second
        blocks[:, at : at + LANES] = by[:BLOCK].astype(BF16)
        blocks[:, at + LANES : at + HALF_BLOCKS] = by[BLOCK:].astype(BF16)
        return first + second

    def write_note():
        load_ends.wait()
        load_handed.wait()
        slots = jnp.sum((note[0:6] > 0).astype(F32), axis=0, keepdims=True)
        slots = jnp.sum(slots, axis=1, keepdims=True) + (note[0:1, 0:1] == 0).astype(F32)
        note[6:7] = jnp.broadcast_to(slots.astype(jnp.int32), (1, LANES))
        note[7:8] = jnp.full((1, LANES), scalars[0], jnp.int32)

    spread = jnp.zeros((CODES, LANES), BF16)
    for i, load in enumerate(load_codes):
        load.wait()
        if i + 1 == len(load_codes):
            write_note()
        for k in range(i * 32, (i + 1) * 32, BLOCK):
            spread = spread + block_counts(own[k : k + BLOCK].astype(F32))
    total = dot_nt(jnp.ones((8, LANES), BF16), spread)[0:1]
    mine[0] = total
    plane[spot] = total

    hears = jnp.where(hub, NY - 1 - y + jnp.where(y > 0, NG * z, 0), NY - y)
    pl.semaphore_wait(barrier, hears + z + jnp.minimum(NSHARDS - 1 - shard, 2))

    def answer(sem, row):
        pl.semaphore_signal(sem, inc=1, device_id=(row, HUB), device_id_type=MESH)

    def spread_to(row, group, batch):
        return pltpu.make_async_remote_copy(
            src_ref=mine.at[0], dst_ref=plane.at[spot], send_sem=p1_send.at[0], recv_sem=p1_recv.at[batch],
            device_id=(row, group), device_id_type=MESH)

    def batch_of(n, send_sem, recv_sem):
        return pltpu.make_async_remote_copy(
            src_ref=plane.at[pl.ds(0, n)], dst_ref=plane.at[pl.ds(0, n)], send_sem=send_sem, recv_sem=recv_sem,
            device_id=(seq, grp), device_id_type=MESH)

    to_hubs = [(y2, spread_to(y2 * NZ + z, HUB, y)) for y2 in range(NY)]
    for y2, copy in to_hubs:
        pl.when(jnp.logical_or(y2 > y, jnp.logical_and(y2 == y, jnp.logical_not(hub))))(copy.start)

    pass_codes = pltpu.make_async_remote_copy(
        src_ref=own, dst_ref=prev, send_sem=pass_send.at[0], recv_sem=pass_recv.at[0],
        device_id=device_of(jnp.minimum(shard + 1, NSHARDS - 1)), device_id_type=MESH)
    pass_note = pltpu.make_async_remote_copy(
        src_ref=note, dst_ref=got, send_sem=pass_send.at[0], recv_sem=pass_recv.at[0],
        device_id=device_of(jnp.minimum(shard + 1, NSHARDS - 1)), device_id_type=MESH)
    pass_tail = pltpu.make_async_remote_copy(
        src_ref=own.at[pl.ds(ROWS // 2, ROWS // 2)], dst_ref=prior, send_sem=pass_send.at[0], recv_sem=pass_recv.at[1],
        device_id=device_of(jnp.minimum(shard + 2, NSHARDS - 1)), device_id_type=MESH)

    @pl.when(shard + 1 < NSHARDS)
    def _():
        pass_note.start()
        pass_codes.start()

    @pl.when(shard + 2 < NSHARDS)
    def _():
        pass_tail.start()

    for z2 in range(NZ - 1):
        pl.when(z2 < z)(functools.partial(answer, ready, y * NZ + z2))
    pl.when(jnp.logical_not(hub))(functools.partial(answer, home, seq))

    enter(3, own[0:32])
    enter(4, own[32:64])

    def climb(z2, g2, kind):
        pltpu.make_async_remote_copy(
            src_ref=sums.at[kind], dst_ref=column.at[z], send_sem=p2_send.at[0], recv_sem=p2_recv.at[0],
            device_id=(y * NZ + z2, g2), device_id_type=MESH).start()

    def send_level():
        pl.semaphore_wait(ready, NG * (NZ - 1 - z))
        for z2 in range(1, NZ):
            @pl.when(z2 > z)
            def _():
                for g2 in range(NG):
                    climb(z2, g2, NG)

    @pl.when(hub)
    def _():
        sums[NG + 1] = jnp.zeros((1, CODES), F32)
        for y2 in range(NY - 1):
            @pl.when(y2 < y)
            def _():
                batch_of(NG, p1_send.at[0], p1_recv.at[y2]).wait_recv()
                part = sums[NG + 1]
                for g2 in range(NG):
                    part = part + plane[y2 * NG + g2]
                sums[NG + 1] = part
        for z2 in range(NZ - 1):
            @pl.when(jnp.logical_and(y > 0, z2 < z))
            def _():
                for g2 in range(NG):
                    climb(z2, g2, NG + 1)
        batch_of(NG - 1, p1_send.at[0], p1_recv.at[y]).wait_recv()
        below = sums[NG + 1]
        for g2 in range(NG):
            sums[g2] = below
            below = below + plane[y * NG + g2]
        sums[NG] = below
        pl.semaphore_wait(home, NG - 1)
        pl.when(jnp.logical_and(y > 0, z < NZ - 1))(send_level)
        for g2 in range(NG):
            if g2 != HUB:
                climb(z, g2, g2)
        column[z] = sums[HUB]

    @pl.when(shard >= 1)
    def _():
        batch_of(4 + 32, p1_send.at[0], pass_recv.at[0]).wait_recv()

    inner = grp > 0
    arrived = jnp.where(inner, got[7:8], 0)
    arrived = jnp.concatenate([arrived, arrived], axis=1)
    behind = jnp.concatenate([got[6:7], got[6:7]], axis=1) - arrived
    kept = note[6:7] - note[7:8]
    kept = jnp.concatenate([kept, kept], axis=1)
    own_line = ends_line(note[...], CAP, SHARD // 256)
    got_line = jnp.where(inner, ends_line(got[...], SLOTS, 0).astype(F32), 0.0).astype(BF16)
    lane = lax.broadcasted_iota(jnp.int32, (1, HAND), 1)
    block_of = block_column()

    known = jnp.where(shard >= 1, prev[...], -1)
    spread = enter(1, known[0:32]) + enter(2, known[32:64])
    before = dot_nt(jnp.ones((8, LANES), BF16), spread)[0:1]

    @pl.when(shard >= 2)
    def _():
        pass_tail.wait_recv()

    enter(0, jnp.where(shard >= 2, prior[...], -1))

    for part in range(2):
        ends = dot(own_line[:, : HAND * (part + 1)], picks(HAND * (part + 1), -arrived, HAND * part))
        if part == 0:
            ends = ends + dot(got_line, picks(SLOTS, behind, 0))
        ends = (ends[0:1] * 256.0 + ends[1:2]).astype(jnp.int32)
        valid = lane + HAND * part - arrived < kept
        upto = (ends + ((shard - 1) * SHARD + 1)).astype(F32)
        inv = jnp.where(valid, 256.0 / upto, 0.0)
        scale = jnp.where(valid, 256.0 / jnp.minimum(upto, float(WINDOW)), 0.0)
        key = ends // BLOCK
        halves = range(1 + 2 * part, 5)
        left, right = HALF_BLOCKS * halves[0], HALF_BLOCKS * 5
        less, same = [], []
        for half in halves:
            there = tall(key - HALF_BLOCKS * (half - 1), HALF_BLOCKS)
            less.append(flag(block_of < there))
            same.append(flag(block_of == there))
        less, same = jnp.concatenate(less, axis=0), jnp.concatenate(same, axis=0)
        upper = dot(counts[:, left:right], less)
        lower = dot(counts[:, left - HALF_BLOCKS : right - HALF_BLOCKS], less)
        tail = dot(counts[:, left - HALF_BLOCKS : left], jnp.ones((HALF_BLOCKS, LANES), BF16))
        found = jnp.concatenate(
            [blocks[:, left:right], blocks[:, left - HALF_BLOCKS : right - HALF_BLOCKS]], axis=0)
        found = dot(found, same)
        place = lax.broadcasted_iota(jnp.int32, (2 * BLOCK, HAND), 0) % BLOCK
        found = jnp.where(place <= ends % BLOCK, found, -1.0)
        for side in range(2):
            at = slice(side * LANES, (side + 1) * LANES)
            high = upper[:, at] + block_counts(found[:BLOCK, at]).astype(F32)
            low = lower[:, at] + block_counts(found[BLOCK:, at]).astype(F32)
            share = (high + tail - low) * scale[:, at]
            gap = share - high * inv[:, at]
            rows = pl.ds(HAND * part + LANES * side, LANES)
            share_ref[rows] = jnp.transpose(share)
            gap_ref[rows] = jnp.transpose(gap)
            inv_ref[rows] = jnp.transpose(jnp.broadcast_to(inv[:, at], (LANES, LANES)))

    pl.when(jnp.logical_and(hub, jnp.logical_and(y == 0, z < NZ - 1)))(send_level)

    for row in range(NY):
        pl.when(jnp.logical_and(y == row, jnp.logical_not(hub)))(
            batch_of(NY - row, p1_send.at[0], p1_recv.at[0]).wait_send)
        if row < NY - 1:
            pl.when(jnp.logical_and(y == row, hub))(batch_of(NY - 1 - row, p1_send.at[0], p1_recv.at[0]).wait_send)

    @pl.when(jnp.logical_and(hub, y > 0))
    def _():
        batch_of(NG * NZ - 1, p2_send.at[0], p1_recv.at[0]).wait_send()

    for row in range(NZ):
        pl.when(jnp.logical_and(hub, jnp.logical_and(y == 0, z == row)))(
            batch_of(NG * (NZ - 1 - row) + NG - 1, p2_send.at[0], p1_recv.at[0]).wait_send)

    @pl.when(shard + 2 < NSHARDS)
    def _():
        batch_of(4 + 32 + 16, pass_send.at[0], p1_recv.at[0]).wait_send()

    @pl.when(shard + 2 == NSHARDS)
    def _():
        batch_of(4 + 32, pass_send.at[0], p1_recv.at[0]).wait_send()

    @pl.when(y > 0)
    def _():
        pl.when(hub)(batch_of(NZ - 1, p1_send.at[0], p2_recv.at[0]).wait_recv)
        pl.when(jnp.logical_not(hub))(batch_of(NZ, p1_send.at[0], p2_recv.at[0]).wait_recv)

    for row in range(NZ):
        first = jnp.logical_and(y == 0, z == row)
        pl.when(jnp.logical_and(first, jnp.logical_not(hub)))(
            batch_of(row + 1, p1_send.at[0], p2_recv.at[0]).wait_recv)
        if row:
            pl.when(jnp.logical_and(first, hub))(batch_of(row, p1_send.at[0], p2_recv.at[0]).wait_recv)

    offset = jnp.zeros((1, CODES), F32)
    for z2 in range(NZ):
        offset = offset + jnp.where(jnp.logical_or(z2 <= z, y > 0), column[z2], 0.0)
    off_ref[0:1] = offset - before
    off_ref[1:2] = offset


def place_kernel(share_ref, gap_ref, inv_ref, off_ref, share_hbm, gap_hbm, buf, sem):
    share = pltpu.make_async_copy(share_ref, share_hbm, sem.at[0])
    share.start()
    copies = [share]
    n = CAP // PIECES
    for i in range(PIECES):
        for k in range(i * n, (i + 1) * n, LANES):
            at = pl.ds(k, LANES)
            offset = off_ref[0:1] if k < HAND else off_ref[1:2]
            inv = inv_ref[at]
            buf[at] = gap_ref[at] - jnp.concatenate([inv, inv], axis=1) * offset
        at = pl.ds(i * n, n)
        copies.append(pltpu.make_async_copy(buf.at[at], gap_hbm.at[at], sem.at[1 + i]))
        copies[-1].start()
    for copy in copies:
        copy.wait()


def local(event_codes, window_ends, window_count, handed):
    vmem = pl.BlockSpec(memory_space=pltpu.VMEM)
    hbm = pl.BlockSpec(memory_space=pl.ANY)
    far = pl.BlockSpec(memory_space=pltpu.HBM)
    dma = pltpu.SemaphoreType.DMA

    def stay(array):
        return pltpu.with_memory_space_constraint(array, pltpu.HBM)

    tallies = pl.pallas_call(
        tally_kernel,
        out_shape=(
            jax.ShapeDtypeStruct((CAP, CODES), F32),
            jax.ShapeDtypeStruct((CAP, CODES), F32),
            jax.ShapeDtypeStruct((CAP, LANES), F32),
            jax.ShapeDtypeStruct((8, CODES), F32),
        ),
        in_specs=[far] * 3,
        out_specs=(vmem,) * 4,
        scratch_shapes=[
            pltpu.VMEM((ROWS, LANES), jnp.int32),
            pltpu.VMEM((ROWS, LANES), jnp.int32),
            pltpu.VMEM((ROWS // 2, LANES), jnp.int32),
            pltpu.VMEM((8, LANES), jnp.int32),
            pltpu.VMEM((8, LANES), jnp.int32),
            pltpu.VMEM((1, 1, CODES), F32),
            pltpu.VMEM((NZ * NG, 1, CODES), F32),
            pltpu.VMEM((NG + 2, 1, CODES), F32),
            pltpu.VMEM((NZ, 1, CODES), F32),
            pltpu.VMEM((CODES, 5 * HALF_BLOCKS), BF16),
            pltpu.VMEM((BLOCK, 5 * HALF_BLOCKS), BF16),
            pltpu.SMEM((1,), jnp.int32),
            dma((2 + ROWS // 32,)), dma((1,)), dma((NY,)), dma((1,)), dma((1,)), dma((1,)), dma((2,)),
            pltpu.SemaphoreType.REGULAR, pltpu.SemaphoreType.REGULAR,
        ],
        compiler_params=pltpu.CompilerParams(
            collective_id=0, has_side_effects=True, vmem_limit_bytes=32 * 2**20),
        name="tally",
    )(stay(event_codes.reshape(ROWS, LANES)), stay(window_ends.reshape(SLOTS // LANES, LANES)), handed)
    return pl.pallas_call(
        place_kernel,
        out_shape=(jax.ShapeDtypeStruct((CAP, CODES), F32),) * 2,
        in_specs=[vmem] * 4,
        out_specs=(hbm, hbm),
        scratch_shapes=[pltpu.VMEM((CAP, CODES), F32), dma((1 + PIECES,))],
        compiler_params=pltpu.CompilerParams(vmem_limit_bytes=16 * 2**20),
        name="place",
    )(*tallies)


def solution(mesh):
    both = ("seq", "grp")
    return jax.shard_map(
        local,
        mesh=mesh,
        in_specs=(P(both), P(both), P(both), P(both)),
        out_specs=(P(both, None), P(both, None)),
        check_vma=False,
    )
```
